32 devices in a mesh: gx: 4 (over x, core), gy: 4 (over z), gz: 2 (over y).
Axes of the slice: x: 2, y: 2, z: 4, core: 2. Of those that a mesh axis runs over, the one named last changes fastest.
Arguments:
- orbitals: float32 [16, 48, 48, 256], P(None, 'gx', 'gy', 'gz'), may hold values from -6 to 6
- potential: float32 [48, 48, 256], P('gx', 'gy', 'gz'), may hold values from 0 to 2
Outputs:
- filtered: float32 [16, 48, 48, 256], P(None, 'gx', 'gy', 'gz')
The draws below stay inside these ranges and needn't reach their ends.
All inputs are finite; a program needn't handle non-finite values.
Results may differ from the reference program's by a relative error of at most 0.00002.
Values sent between devices are 32-bit elements; how exact they have to be, the bound alone decides.
A program may use at most 64 MiB of HBM per device.

```python
import jax
import jax.numpy as jnp
from jax import lax

BANDS = 16
DEGREE = 2
NX = 48
NY = 48
NZ = 256


def level_of(key, dims, cuts, least, high):
    loudness = 1.0
    for axis_at, blocks in cuts:
        heights = jax.random.uniform(jax.random.fold_in(jax.random.fold_in(key, 6), axis_at), (blocks,), jnp.float32, least / len(cuts), high / len(cuts))
        loudness = loudness * jnp.repeat(jnp.exp(heights), dims[axis_at] // blocks).reshape((-1,) + (1,) * (len(dims) - 1 - axis_at))
    return loudness


def normal_values(stream_key, dims, scale, most, split=(), kind=jnp.bfloat16):
    level = level_of(stream_key, dims, split, -0.22, 0.18) if split else 1.0
    array = jax.random.normal(stream_key, dims, jnp.float32) * scale * level
    return jnp.minimum(jnp.maximum(array, -most), most).astype(kind)


def setup_inputs(seed: int = 0) -> dict:
    streams_of = jax.random.split(jax.random.key(seed), 3)
    return {
        "orbitals": normal_values(streams_of[0], (BANDS, NX, NY, NZ), 1.0, 6.0, ((1, 4), (2, 4), (3, 2)), jnp.float32),
        "potential": jnp.clip(2.0 * jax.random.uniform(streams_of[1], (NX, NY, NZ), jnp.float32) ** level_of(streams_of[1], (NX, NY, NZ), ((0, 4), (1, 4), (2, 2)), -0.2, 0.2), 0.0, 2.0),
    }


SECOND = (-5369.0 / 1800.0, 12.0 / 7.0, -15.0 / 56.0, 10.0 / 189.0, -1.0 / 112.0, 2.0 / 1925.0, -1.0 / 16632.0)
FIRST = (6.0 / 7.0, -15.0 / 56.0, 5.0 / 63.0, -1.0 / 56.0, 3.0 / 385.0, -1.0 / 792.0)
METRIC = ((1.0, 0.25, 0.15), (0.25, 1.0, 0.2), (0.15, 0.2, 1.0))
CENTER = 10.5
HALF_WIDTH = 9.5


def window(values, starts, lengths):
    leading = values.ndim - 3
    starts_full = (0,) * leading + tuple(starts)
    limits = tuple(values.shape[:leading]) + tuple(s + l for s, l in zip(starts, lengths))
    return lax.slice(values, starts_full, limits)


def apply_operator(padded, potential):
    lengths = [padded.shape[i + 1] - 12 for i in range(3)]
    centre = window(padded, (6, 6, 6), lengths)
    summed = METRIC[0][0] * 0.0 * centre
    for d in range(3):
        second = SECOND[0] * centre
        for k in range(1, 7):
            forward = [6, 6, 6]
            forward[d] += k
            backward = [6, 6, 6]
            backward[d] -= k
            second = second + SECOND[k] * (window(padded, forward, lengths) + window(padded, backward, lengths))
        summed = summed + METRIC[d][d] * second
    for d, e in ((0, 1), (0, 2), (1, 2)):
        widened = list(lengths)
        widened[d] += 12
        partial_sum = None
        for k in range(1, 7):
            forward = [6, 6, 6]
            forward[d] = 0
            forward[e] += k
            backward = [6, 6, 6]
            backward[d] = 0
            backward[e] -= k
            term = FIRST[k - 1] * (window(padded, forward, widened) - window(padded, backward, widened))
            partial_sum = term if partial_sum is None else partial_sum + term
        crossed = None
        for k in range(1, 7):
            forward = [0, 0, 0]
            forward[d] = 6 + k
            backward = [0, 0, 0]
            backward[d] = 6 - k
            term = FIRST[k - 1] * (window(partial_sum, forward, lengths) - window(partial_sum, backward, lengths))
            crossed = term if crossed is None else crossed + term
        summed = summed + 2.0 * METRIC[d][e] * crossed
    return -0.5 * summed + potential[None] * centre


def reference(orbitals, potential):
    previous = jnp.zeros_like(orbitals)
    current = orbitals
    for degree_step in range(DEGREE):
        padded = jnp.pad(current, ((0, 0), (6, 6), (6, 6), (6, 6)), mode="wrap")
        applied = apply_operator(padded, potential)
        factor = 1.0 if degree_step == 0 else 2.0
        carry_factor = 0.0 if degree_step == 0 else 1.0
        following = factor * (applied - CENTER * current) / HALF_WIDTH - carry_factor * previous
        previous = current
        current = following
    return current
```

```python
import functools
import math

import jax
import jax.numpy as jnp
import numpy as np
from jax import lax
from jax.experimental import pallas as pl
from jax.experimental.pallas import tpu as pltpu
from jax.sharding import PartitionSpec as P

DEGREE = 2
SECOND = (
    -5369.0 / 1800.0,
    12.0 / 7.0,
    -15.0 / 56.0,
    10.0 / 189.0,
    -1.0 / 112.0,
    2.0 / 1925.0,
    -1.0 / 16632.0,
)
FIRST = (6.0 / 7.0, -15.0 / 56.0, 5.0 / 63.0, -1.0 / 56.0, 3.0 / 385.0, -1.0 / 792.0)
METRIC = ((1.0, 0.25, 0.15), (0.25, 1.0, 0.2), (0.15, 0.2, 1.0))
CENTER = 10.5
HALF_WIDTH = 9.5
R = 6
Y0 = 8
MESH = pl.DeviceIdType.MESH


def z_matrices(bz):
    w = np.zeros((bz + 128, 2 * bz), np.float64)

    def row(p):
        return p if 0 <= p < bz else (bz + 8 + p if p < 0 else p + 8)

    for n in range(bz):
        for k in range(1, R + 1):
            w[row(n + k), n] += FIRST[k - 1]
            w[row(n - k), n] -= FIRST[k - 1]
            w[row(n + k), bz + n] += -0.5 * METRIC[2][2] * SECOND[k]
            w[row(n - k), bz + n] += -0.5 * METRIC[2][2] * SECOND[k]
    high = w.astype(np.float32).astype(jnp.bfloat16)
    low = (w - high.astype(np.float64)).astype(np.float32).astype(jnp.bfloat16)
    return jnp.asarray(high), jnp.asarray(low)


def kernel(
    gx, gy, gz, bx, by,
    orb, pot, whi_ref, wlo_ref, out,
    vin, pin, p_ref, v0, v1, a_ref, c0, c1, s_ref, obuf, ebuf, hbuf,
    isend, irecv, psend, precv, qsend, qrecv, hsend, hrecv, osend, orecv, lsem,
):
    bz = orb.shape[-1]
    nx, ny = gx * bx, gy * by
    group = 8 // math.gcd(by, 8)
    rows = bx * ny
    padded_rows = ebuf.shape[-1]
    cx, cy, cz = lax.axis_index("gx"), lax.axis_index("gy"), lax.axis_index("gz")
    band = cx * gy + cy
    zl, zr = lax.rem(cz + gz - 1, gz), lax.rem(cz + 1, gz)
    odd = lax.rem(cx, 2)
    chip = cx - odd
    partner = chip + 1 - odd

    def across(d):
        ty, bit = cy, 1
        while bit <= d:
            if d & bit:
                ty = ty + bit - 2 * bit * lax.rem(lax.div(cy, bit), 2)
            bit *= 2
        return ty

    far_first = list(range(gy - 1, 0, -1))

    barrier = pltpu.get_barrier_semaphore()
    for dx in range(gx):
        for dy in range(gy):
            if dx or dy:
                pl.semaphore_signal(
                    barrier, inc=1,
                    device_id=(lax.rem(cx + dx, gx), lax.rem(cy + dy, gy), cz),
                    device_id_type=MESH,
                )
    for z in (zl, zr):
        pl.semaphore_signal(barrier, inc=1, device_id=(cx, cy, z), device_id_type=MESH)
    pl.semaphore_wait(barrier, gx * gy + 1)

    own_pot = pltpu.make_async_copy(pot, pin.at[cx, cy], lsem.at[1])
    own_pot.start()
    gathers = [own_pot]
    for dy in far_first:
        copy = pltpu.make_async_remote_copy(
            pot, pin.at[cx, cy], psend.at[dy], precv.at[dy],
            device_id=(cx, across(dy), cz), device_id_type=MESH,
        )
        copy.start()
        gathers.append(copy)

    own_band = pltpu.make_async_copy(orb.at[band], vin.at[cx, cy], lsem.at[0])
    bands_out = []

    def send_band(n, tx, ty):
        copy = pltpu.make_async_remote_copy(
            orb.at[tx * gy + ty], vin.at[cx, cy], isend.at[n], irecv.at[cx, cy],
            device_id=(tx, ty, cz), device_id_type=MESH,
        )
        copy.start()
        bands_out.append(copy)

    def send_group(g):
        for d in far_first + [0]:
            for i in range(gx // 2):
                if i or d:
                    n = (g * (gx // 2) + i) * gy + d
                    send_band(n, lax.rem(chip + 2 * i + g, gx), across(d))

    def wait_block(sx, own):
        for d in range(gy):
            sy = across(d)
            if own and d == 0:
                own_band.wait()
            else:
                pltpu.make_async_remote_copy(
                    orb.at[band], vin.at[sx, sy], isend.at[0], irecv.at[sx, sy],
                    device_id=(partner, cy, cz), device_id_type=MESH,
                ).wait_recv()

    spread_steps = []
    d = gx // 2
    while d:
        spread_steps.append(d)
        d //= 2
    held = [cx]
    spread_count = [0]

    def spread(d):
        bit = lax.rem(lax.div(cx, d), 2)
        hop = d - 2 * d * bit
        copies = []
        for r in list(held):
            i = spread_count[0]
            spread_count[0] += 1
            copy = pltpu.make_async_remote_copy(
                pin.at[r], pin.at[r], qsend.at[i], qrecv.at[i],
                device_id=(cx + hop, cy, cz), device_id_type=MESH,
            )
            copy.start()
            copies.append(copy)
            held.append(r + hop)
        return copies

    def wrap_y(ref, x):
        ref[x, pl.ds(Y0 - R, R), :] = ref[x, pl.ds(Y0 + ny - R, R), :]
        ref[x, pl.ds(Y0 + ny, R), :] = ref[x, pl.ds(Y0, R), :]

    def wrap_x(ref, sx):
        @pl.when(sx == 0)
        def _():
            ref[pl.ds(nx + R, R)] = ref[pl.ds(R, R)]

        @pl.when(sx == gx - 1)
        def _():
            ref[pl.ds(0, R)] = ref[pl.ds(nx, R)]

    def pieces(ref, sx, i):
        at = pl.multiple_of(i * group * by, 8)
        for sy in range(gy):
            got = ref[sx, sy, pl.ds(at, group * by), :]
            for j in range(group):
                yield sy, j, got[j * by : (j + 1) * by]

    def assemble(sx):
        @pl.loop(0, bx // group)
        def _(i):
            x = sx * bx + i * group + R
            for sy, j, piece in pieces(vin, sx, i):
                v0[x + j, pl.ds(Y0 + sy * by, by), :] = piece
            for j in range(group):
                wrap_y(v0, x + j)
        wrap_x(v0, sx)

    def assemble_potential():
        for sx in range(gx):
            @pl.loop(0, bx // group)
            def _(i):
                x = sx * bx + i * group
                for sy, j, piece in pieces(pin, sx, i):
                    p_ref[x + j, pl.ds(sy * by, by), :] = piece + (-1.5 * SECOND[0] - CENTER)

    def send_edges(step, v, sx, t):
        vals = v[pl.ds(sx * bx + R, bx), pl.ds(Y0, ny), :].reshape(rows, bz)
        if padded_rows > rows:
            vals = jnp.concatenate([vals, jnp.zeros((padded_rows - rows, bz), jnp.float32)], axis=0)
        for i in range(padded_rows // 128):
            turned = vals[i * 128 : (i + 1) * 128].T
            ebuf[step, t, 0, :, pl.ds(i * 128, 128)] = turned[:8]
            ebuf[step, t, 1, :, pl.ds(i * 128, 128)] = turned[bz - 8 :]
        copies = []
        for side, z in ((0, zl), (1, zr)):
            copy = pltpu.make_async_remote_copy(
                ebuf.at[step, t, side], hbuf.at[step, t, 1 - side],
                hsend.at[step, t, side], hrecv.at[step, t, 1 - side],
                device_id=(cx, cy, z), device_id_type=MESH,
            )
            copy.start()
            copies.append(copy)
        return copies

    def y_pass(v, c_ref, sx):
        @pl.loop(0, bx)
        def _(i):
            x = sx * bx + i
            first = second = None
            for k in range(1, R + 1):
                up = v[x + R, pl.ds(Y0 + k, ny), :]
                down = v[x + R, pl.ds(Y0 - k, ny), :]
                f = (-METRIC[0][1] * FIRST[k - 1]) * (up - down)
                s = (-0.5 * METRIC[1][1] * SECOND[k]) * (up + down)
                first = f if first is None else first + f
                second = s if second is None else second + s
            c_ref[x + R] = first
            s_ref[x] = second

    def z_pass(step, v, c_ref, sx, t):
        vals = v[pl.ds(sx * bx + R, bx), pl.ds(Y0, ny), :].reshape(rows, bz)
        sides = []
        for i in range(padded_rows // 128):
            block = jnp.concatenate(
                [
                    hbuf[step, t, 0, :, pl.ds(i * 128, 128)],
                    hbuf[step, t, 1, :, pl.ds(i * 128, 128)],
                    jnp.zeros((112, 128), jnp.float32),
                ],
                axis=0,
            )
            sides.append(block.T)
        full = jnp.concatenate([vals, jnp.concatenate(sides, axis=0)[:rows]], axis=1)
        high = full.astype(jnp.bfloat16)
        low = (full - high.astype(jnp.float32)).astype(jnp.bfloat16)
        dot = functools.partial(jnp.dot, preferred_element_type=jnp.float32)
        whi = whi_ref[...]
        got = dot(high, whi) + (dot(low, whi) + dot(high, wlo_ref[...]))
        a = got[:, :bz].reshape(bx, ny, bz)
        s_ref[pl.ds(sx * bx, bx)] += got[:, bz:].reshape(bx, ny, bz)
        c_ref[pl.ds(sx * bx + R, bx)] += (-METRIC[0][2]) * a
        a_ref[pl.ds(sx * bx, bx), pl.ds(Y0, ny), :] = a
        for i in range(bx):
            wrap_y(a_ref, sx * bx + i)
        wrap_x(c_ref, sx)

    def x_row(v, c_ref, x):
        total = s_ref[x] + p_ref[x] * v[x + R, pl.ds(Y0, ny), :]
        for k in range(1, R + 1):
            total = total + (-0.5 * METRIC[0][0] * SECOND[k]) * (
                v[x + R + k, pl.ds(Y0, ny), :] + v[x + R - k, pl.ds(Y0, ny), :]
            )
            total = total + FIRST[k - 1] * (c_ref[x + R + k] - c_ref[x + R - k])
            total = total + (-METRIC[1][2] * FIRST[k - 1]) * (
                a_ref[x, pl.ds(Y0 + k, ny), :] - a_ref[x, pl.ds(Y0 - k, ny), :]
            )
        return total

    def wait_all(copies):
        for copy in copies:
            copy.wait()

    block = [lax.rem(cx + gx + t - 2 * t * odd, gx) for t in range(gx)]
    second_edges = {}

    def first_x_pass(t):
        sx = block[t]

        @pl.loop(0, bx)
        def _(i):
            x = sx * bx + i
            v1[x + R, pl.ds(Y0, ny), :] = (1.0 / HALF_WIDTH) * x_row(v0, c0, x)
            wrap_y(v1, x + R)
        wrap_x(v1, sx)
        second_edges[t] = send_edges(1, v1, sx, t)
        y_pass(v1, c1, sx)

    own_band.start()
    send_band(0, partner, cy)
    send_group(0)
    wait_all(gathers)
    doing = spread(spread_steps[0])
    send_group(1)
    first_edges = []
    for t in range(gx):
        wait_block(block[t], t == 0)
        assemble(block[t])
        first_edges.append(send_edges(0, v0, block[t], t))
        y_pass(v0, c0, block[t])
        if 1 <= t < gx - 1:
            wait_all(doing)
            doing = spread(spread_steps[t]) if t < len(spread_steps) else []
        if t == gx - 1:
            wait_all(doing)
            assemble_potential()
        if t >= 1:
            wait_all(first_edges[t - 1])
            z_pass(0, v0, c0, block[t - 1], t - 1)
    for t in range(1, gx - 2):
        first_x_pass(t)
    wait_all(first_edges[gx - 1])
    z_pass(0, v0, c0, block[gx - 1], gx - 1)
    late = [gx - 2, gx - 1, 0]
    for t in late:
        first_x_pass(t)

    outgoing = []

    def last_x_pass(t):
        sx = block[t]

        @pl.loop(0, bx // group)
        def _(i):
            got = []
            for j in range(group):
                x = sx * bx + i * group + j
                got.append(
                    (2.0 / HALF_WIDTH) * x_row(v1, c1, x) - v0[x + R, pl.ds(Y0, ny), :]
                )
            at = pl.multiple_of(i * group * by, 8)
            for sy in range(gy):
                obuf[sx, sy, pl.ds(at, group * by), :] = jnp.concatenate(
                    [g[sy * by : (sy + 1) * by] for g in got], axis=0
                )

        for dy in far_first + [0]:
            ty = across(dy)
            n = t * gy + dy
            if n == 0:
                copy = pltpu.make_async_copy(obuf.at[sx, ty], out.at[band], lsem.at[2])
            else:
                copy = pltpu.make_async_remote_copy(
                    obuf.at[sx, ty], out.at[band], osend.at[n], orecv.at[n],
                    device_id=(sx, ty, cz), device_id_type=MESH,
                )
            copy.start()
            outgoing.append(copy)

    ready = list(range(1, gx - 2)) + late
    done = []
    for t in ready:
        wait_all(second_edges[t])
        z_pass(1, v1, c1, block[t], t)
        done.append(t)
        for u in range(gx):
            near = {u, (u + 1) % gx, (u - 1) % gx}
            if near <= set(done) and t in near:
                last_x_pass(u)
    wait_all(outgoing)
    for copy in bands_out:
        copy.wait_send()


def local(sizes, orbitals, potential):
    gx, gy, gz = sizes
    bands, bx, by, bz = orbitals.shape
    nx, ny = gx * bx, gy * by
    assert bands == gx * gy and gz > 1 and gx >= 4 and gx & (gx - 1) == 0
    f32 = jnp.float32
    whi, wlo = z_matrices(bz)
    anywhere = pl.BlockSpec(memory_space=pl.ANY)
    vmem = pl.BlockSpec(memory_space=pltpu.VMEM)
    dma = pltpu.SemaphoreType.DMA
    edge = (DEGREE, gx, 2, 8, (bx * ny + 127) // 128 * 128)
    out = pl.pallas_call(
        functools.partial(kernel, gx, gy, gz, bx, by),
        out_shape=jax.ShapeDtypeStruct((bands, bx * by, bz), f32),
        in_specs=[anywhere, anywhere, vmem, vmem],
        out_specs=anywhere,
        scratch_shapes=[
            pltpu.VMEM((gx, gy, bx * by, bz), f32),
            pltpu.VMEM((gx, gy, bx * by, bz), f32),
            pltpu.VMEM((nx, ny, bz), f32),
            pltpu.VMEM((nx + 2 * R, ny + 16, bz), f32),
            pltpu.VMEM((nx + 2 * R, ny + 16, bz), f32),
            pltpu.VMEM((nx, ny + 16, bz), f32),
            pltpu.VMEM((nx + 2 * R, ny, bz), f32),
            pltpu.VMEM((nx + 2 * R, ny, bz), f32),
            pltpu.VMEM((nx, ny, bz), f32),
            pltpu.VMEM((gx, gy, bx * by, bz), f32),
            pltpu.VMEM(edge, f32),
            pltpu.VMEM(edge, f32),
            dma((gx * gy,)), dma((gx, gy)),
            dma((gy,)), dma((gy,)),
            dma((gx,)), dma((gx,)),
            dma((DEGREE, gx, 2)), dma((DEGREE, gx, 2)),
            dma((gx * gy,)), dma((gx * gy,)),
            dma((3,)),
        ],
        compiler_params=pltpu.CompilerParams(
            collective_id=0, has_side_effects=True, vmem_limit_bytes=48 * 1024 * 1024
        ),
    )(
        orbitals.reshape(bands, bx * by, bz),
        potential.reshape(bx * by, bz),
        whi,
        wlo,
    )
    return out.reshape(bands, bx, by, bz)


def solution(mesh):
    sizes = tuple(mesh.shape[a] for a in ("gx", "gy", "gz"))
    return jax.shard_map(
        functools.partial(local, sizes),
        mesh=mesh,
        in_specs=(P(None, "gx", "gy", "gz"), P("gx", "gy", "gz")),
        out_specs=P(None, "gx", "gy", "gz"),
        check_vma=False,
    )
```

```python
import functools
import math

import jax
import jax.numpy as jnp
import numpy as np
from jax import lax
from jax.experimental import pallas as pl
from jax.experimental.pallas import tpu as pltpu
from jax.sharding import PartitionSpec as P

DEGREE = 2
SECOND = (
    -5369.0 / 1800.0,
    12.0 / 7.0,
    -15.0 / 56.0,
    10.0 / 189.0,
    -1.0 / 112.0,
    2.0 / 1925.0,
    -1.0 / 16632.0,
)
FIRST = (6.0 / 7.0, -15.0 / 56.0, 5.0 / 63.0, -1.0 / 56.0, 3.0 / 385.0, -1.0 / 792.0)
METRIC = ((1.0, 0.25, 0.15), (0.25, 1.0, 0.2), (0.15, 0.2, 1.0))
CENTER = 10.5
HALF_WIDTH = 9.5
R = 6
Y0 = 8
MESH = pl.DeviceIdType.MESH


def z_matrices(bz):
    w = np.zeros((bz + 128, 2 * bz), np.float64)

    def row(p):
        return p if 0 <= p < bz else (bz + 8 + p if p < 0 else p + 8)

    for n in range(bz):
        for k in range(1, R + 1):
            w[row(n + k), n] += FIRST[k - 1]
            w[row(n - k), n] -= FIRST[k - 1]
            w[row(n + k), bz + n] += -0.5 * METRIC[2][2] * SECOND[k]
            w[row(n - k), bz + n] += -0.5 * METRIC[2][2] * SECOND[k]
    high = w.astype(np.float32).astype(jnp.bfloat16)
    low = (w - high.astype(np.float64)).astype(np.float32).astype(jnp.bfloat16)
    return jnp.asarray(high), jnp.asarray(low)


def kernel(
    gx, gy, gz, bx, by,
    orb, pot, whi_ref, wlo_ref, out,
    vin, pin, p_ref, v0, v1, a_ref, c0, c1, s_ref, obuf, ebuf, hbuf,
    isend, irecv, psend, precv, qsend, qrecv, hsend, hrecv, osend, orecv, lsem,
):
    bz = orb.shape[-1]
    nx, ny = gx * bx, gy * by
    group = 8 // math.gcd(by, 8)
    rows = bx * ny
    padded_rows = ebuf.shape[-1]
    cx, cy, cz = lax.axis_index("gx"), lax.axis_index("gy"), lax.axis_index("gz")
    band = cx * gy + cy
    zl, zr = lax.rem(cz + gz - 1, gz), lax.rem(cz + 1, gz)
    odd = lax.rem(cx, 2)
    chip = cx - odd
    partner = chip + 1 - odd

    def across(d):
        ty, bit = cy, 1
        while bit <= d:
            if d & bit:
                ty = ty + bit - 2 * bit * lax.rem(lax.div(cy, bit), 2)
            bit *= 2
        return ty

    far_first = list(range(gy - 1, 0, -1))

    barrier = pltpu.get_barrier_semaphore()
    for dx in range(gx):
        for dy in range(gy):
            if dx or dy:
                pl.semaphore_signal(
                    barrier, inc=1,
                    device_id=(lax.rem(cx + dx, gx), lax.rem(cy + dy, gy), cz),
                    device_id_type=MESH,
                )
    for z in (zl, zr):
        pl.semaphore_signal(barrier, inc=1, device_id=(cx, cy, z), device_id_type=MESH)
    pl.semaphore_wait(barrier, gx * gy + 1)

    own_pot = pltpu.make_async_copy(pot, pin.at[cx, cy], lsem.at[1])
    masks = []
    m = gy - 1
    while m:
        masks.append(m)
        m //= 2
    mates = [lax.rem(cx + 2 * i, gx) for i in range(1, gx // 2)]
    pot_out = []

    def send_pot(src, x, y, target):
        copy = pltpu.make_async_remote_copy(
            src, pin.at[x, y], psend.at[len(pot_out)], precv.at[x, y],
            device_id=target + (cz,), device_id_type=MESH,
        )
        copy.start()
        pot_out.append(copy)

    def wait_pot(x, y):
        pltpu.make_async_remote_copy(
            pot, pin.at[x, y], psend.at[0], precv.at[x, y],
            device_id=(partner, cy, cz), device_id_type=MESH,
        ).wait_recv()

    def share_pot():
        copies = []
        for i, x in enumerate([cx] + mates):
            copy = pltpu.make_async_remote_copy(
                pin.at[x], pin.at[x], qsend.at[i], qrecv.at[i],
                device_id=(partner, cy, cz), device_id_type=MESH,
            )
            copy.start()
            copies.append(copy)
        return copies

    own_band = pltpu.make_async_copy(orb.at[band], vin.at[cx, cy], lsem.at[0])
    bands_out = []

    def send_band(n, tx, ty):
        copy = pltpu.make_async_remote_copy(
            orb.at[tx * gy + ty], vin.at[cx, cy], isend.at[n], irecv.at[cx, cy],
            device_id=(tx, ty, cz), device_id_type=MESH,
        )
        copy.start()
        bands_out.append(copy)

    def send_group(g, pairs, ds):
        for d in ds:
            for i in pairs:
                if i or d:
                    n = (g * (gx // 2) + i) * gy + d
                    send_band(n, lax.rem(chip + 2 * i + g, gx), across(d))

    def wait_block(sx, own):
        for d in range(gy):
            sy = across(d)
            if own and d == 0:
                own_band.wait()
            else:
                pltpu.make_async_remote_copy(
                    orb.at[band], vin.at[sx, sy], isend.at[0], irecv.at[sx, sy],
                    device_id=(partner, cy, cz), device_id_type=MESH,
                ).wait_recv()

    def wrap_y(ref, x):
        ref[x, pl.ds(Y0 - R, R), :] = ref[x, pl.ds(Y0 + ny - R, R), :]
        ref[x, pl.ds(Y0 + ny, R), :] = ref[x, pl.ds(Y0, R), :]

    def wrap_x(ref, sx):
        @pl.when(sx == 0)
        def _():
            ref[pl.ds(nx + R, R)] = ref[pl.ds(R, R)]

        @pl.when(sx == gx - 1)
        def _():
            ref[pl.ds(0, R)] = ref[pl.ds(nx, R)]

    def pieces(ref, sx, i):
        at = pl.multiple_of(i * group * by, 8)
        for sy in range(gy):
            got = ref[sx, sy, pl.ds(at, group * by), :]
            for j in range(group):
                yield sy, j, got[j * by : (j + 1) * by]

    def assemble(sx):
        @pl.loop(0, bx // group)
        def _(i):
            x = sx * bx + i * group + R
            for sy, j, piece in pieces(vin, sx, i):
                v0[x + j, pl.ds(Y0 + sy * by, by), :] = piece
            for j in range(group):
                wrap_y(v0, x + j)
        wrap_x(v0, sx)

    def assemble_potential():
        for sx in range(gx):
            @pl.loop(0, bx // group)
            def _(i):
                x = sx * bx + i * group
                for sy, j, piece in pieces(pin, sx, i):
                    p_ref[x + j, pl.ds(sy * by, by), :] = piece + (-1.5 * SECOND[0] - CENTER)

    def send_edges(step, v, sx, t):
        vals = v[pl.ds(sx * bx + R, bx), pl.ds(Y0, ny), :].reshape(rows, bz)
        if padded_rows > rows:
            vals = jnp.concatenate([vals, jnp.zeros((padded_rows - rows, bz), jnp.float32)], axis=0)
        for i in range(padded_rows // 128):
            turned = vals[i * 128 : (i + 1) * 128].T
            ebuf[step, t, 0, :, pl.ds(i * 128, 128)] = turned[:8]
            ebuf[step, t, 1, :, pl.ds(i * 128, 128)] = turned[bz - 8 :]
        copies = []
        for side, z in ((0, zl), (1, zr)):
            copy = pltpu.make_async_remote_copy(
                ebuf.at[step, t, side], hbuf.at[step, t, 1 - side],
                hsend.at[step, t, side], hrecv.at[step, t, 1 - side],
                device_id=(cx, cy, z), device_id_type=MESH,
            )
            copy.start()
            copies.append(copy)
        return copies

    def y_pass(v, c_ref, sx):
        @pl.loop(0, bx)
        def _(i):
            x = sx * bx + i
            first = second = None
            for k in range(1, R + 1):
                up = v[x + R, pl.ds(Y0 + k, ny), :]
                down = v[x + R, pl.ds(Y0 - k, ny), :]
                f = (-METRIC[0][1] * FIRST[k - 1]) * (up - down)
                s = (-0.5 * METRIC[1][1] * SECOND[k]) * (up + down)
                first = f if first is None else first + f
                second = s if second is None else second + s
            c_ref[x + R] = first
            s_ref[x] = second

    def z_pass(step, v, c_ref, sx, t):
        vals = v[pl.ds(sx * bx + R, bx), pl.ds(Y0, ny), :].reshape(rows, bz)
        sides = []
        for i in range(padded_rows // 128):
            block = jnp.concatenate(
                [
                    hbuf[step, t, 0, :, pl.ds(i * 128, 128)],
                    hbuf[step, t, 1, :, pl.ds(i * 128, 128)],
                    jnp.zeros((112, 128), jnp.float32),
                ],
                axis=0,
            )
            sides.append(block.T)
        full = jnp.concatenate([vals, jnp.concatenate(sides, axis=0)[:rows]], axis=1)
        high = full.astype(jnp.bfloat16)
        low = (full - high.astype(jnp.float32)).astype(jnp.bfloat16)
        dot = functools.partial(jnp.dot, preferred_element_type=jnp.float32)
        whi = whi_ref[...]
        got = dot(high, whi) + (dot(low, whi) + dot(high, wlo_ref[...]))
        a = got[:, :bz].reshape(bx, ny, bz)
        s_ref[pl.ds(sx * bx, bx)] += got[:, bz:].reshape(bx, ny, bz)
        c_ref[pl.ds(sx * bx + R, bx)] += (-METRIC[0][2]) * a
        a_ref[pl.ds(sx * bx, bx), pl.ds(Y0, ny), :] = a
        for i in range(bx):
            wrap_y(a_ref, sx * bx + i)
        wrap_x(c_ref, sx)

    def x_row(v, c_ref, x):
        total = s_ref[x] + p_ref[x] * v[x + R, pl.ds(Y0, ny), :]
        for k in range(1, R + 1):
            total = total + (-0.5 * METRIC[0][0] * SECOND[k]) * (
                v[x + R + k, pl.ds(Y0, ny), :] + v[x + R - k, pl.ds(Y0, ny), :]
            )
            total = total + FIRST[k - 1] * (c_ref[x + R + k] - c_ref[x + R - k])
            total = total + (-METRIC[1][2] * FIRST[k - 1]) * (
                a_ref[x, pl.ds(Y0 + k, ny), :] - a_ref[x, pl.ds(Y0 - k, ny), :]
            )
        return total

    def wait_all(copies):
        for copy in copies:
            copy.wait()

    block = [lax.rem(cx + gx + t - 2 * t * odd, gx) for t in range(gx)]
    second_edges = {}

    def first_x_pass(t):
        sx = block[t]

        @pl.loop(0, bx)
        def _(i):
            x = sx * bx + i
            v1[x + R, pl.ds(Y0, ny), :] = (1.0 / HALF_WIDTH) * x_row(v0, c0, x)
            wrap_y(v1, x + R)
        wrap_x(v1, sx)
        second_edges[t] = send_edges(1, v1, sx, t)
        y_pass(v1, c1, sx)

    far = list(range(gy - 1, gy // 2 - 1, -1))
    near = list(range(gy // 2 - 1, -1, -1))
    others = list(range(1, gx // 2))

    own_pot.start()
    for d in masks:
        send_pot(pot, cx, cy, (cx, across(d)))
    for x in mates:
        send_pot(pot, cx, cy, (x, cy))
    own_band.start()
    send_band(0, partner, cy)
    send_group(0, [0], far)
    reached = [0]
    for d in masks:
        wait_pot(cx, across(d))
    for x in mates:
        wait_pot(x, cy)
        for d in masks:
            send_pot(pin.at[cx, across(d)], cx, across(d), (x, cy))
    hops = []
    for k, m in enumerate(masks):
        if k:
            hops.append((m, [o for o in reached if o]))
        reached = reached + [o ^ m for o in reached]

    def forward(x, hop):
        m, offsets = hop
        for o in offsets:
            send_pot(pin.at[x, across(o)], x, across(o), (cx, across(m)))

    def arrive(x, hop):
        m, offsets = hop
        for o in offsets:
            wait_pot(x, across(o ^ m))

    for hop in hops[:1]:
        forward(cx, hop)
    send_group(0, others, far + near)
    for k, hop in enumerate(hops):
        if k:
            forward(cx, hop)
        arrive(cx, hop)
    for x in mates:
        for d in masks:
            wait_pot(x, across(d))
        for hop in hops[:1]:
            forward(x, hop)
    send_group(0, [0], near)
    for k, hop in enumerate(hops):
        for x in mates:
            if k:
                forward(x, hop)
            arrive(x, hop)
    own_pot.wait()
    sharing = share_pot()
    send_group(1, [0] + others, near + far)
    first_edges = []
    for t in range(gx):
        wait_block(block[t], t == 0)
        assemble(block[t])
        first_edges.append(send_edges(0, v0, block[t], t))
        y_pass(v0, c0, block[t])
        if t == gx - 1:
            wait_all(sharing)
            assemble_potential()
        if t >= 1:
            wait_all(first_edges[t - 1])
            z_pass(0, v0, c0, block[t - 1], t - 1)
    for t in range(1, gx - 2):
        first_x_pass(t)
    wait_all(first_edges[gx - 1])
    z_pass(0, v0, c0, block[gx - 1], gx - 1)
    late = [gx - 2, gx - 1, 0]
    for t in late:
        first_x_pass(t)

    outgoing = []

    def last_x_pass(t):
        sx = block[t]

        @pl.loop(0, bx // group)
        def _(i):
            got = []
            for j in range(group):
                x = sx * bx + i * group + j
                got.append(
                    (2.0 / HALF_WIDTH) * x_row(v1, c1, x) - v0[x + R, pl.ds(Y0, ny), :]
                )
            at = pl.multiple_of(i * group * by, 8)
            for sy in range(gy):
                obuf[sx, sy, pl.ds(at, group * by), :] = jnp.concatenate(
                    [g[sy * by : (sy + 1) * by] for g in got], axis=0
                )

        for dy in far_first + [0]:
            ty = across(dy)
            n = t * gy + dy
            if n == 0:
                copy = pltpu.make_async_copy(obuf.at[sx, ty], out.at[band], lsem.at[2])
            else:
                copy = pltpu.make_async_remote_copy(
                    obuf.at[sx, ty], out.at[band], osend.at[n], orecv.at[n],
                    device_id=(sx, ty, cz), device_id_type=MESH,
                )
            copy.start()
            outgoing.append(copy)

    ready = list(range(1, gx - 2)) + late
    done = []
    for t in ready:
        wait_all(second_edges[t])
        z_pass(1, v1, c1, block[t], t)
        done.append(t)
        for u in range(gx):
            near = {u, (u + 1) % gx, (u - 1) % gx}
            if near <= set(done) and t in near:
                last_x_pass(u)
    wait_all(outgoing)
    for copy in bands_out + pot_out:
        copy.wait_send()


def local(sizes, orbitals, potential):
    gx, gy, gz = sizes
    bands, bx, by, bz = orbitals.shape
    nx, ny = gx * bx, gy * by
    assert bands == gx * gy and gz > 1 and gx >= 4 and gx & (gx - 1) == 0
    f32 = jnp.float32
    whi, wlo = z_matrices(bz)
    anywhere = pl.BlockSpec(memory_space=pl.ANY)
    vmem = pl.BlockSpec(memory_space=pltpu.VMEM)
    dma = pltpu.SemaphoreType.DMA
    edge = (DEGREE, gx, 2, 8, (bx * ny + 127) // 128 * 128)
    out = pl.pallas_call(
        functools.partial(kernel, gx, gy, gz, bx, by),
        out_shape=jax.ShapeDtypeStruct((bands, bx * by, bz), f32),
        in_specs=[anywhere, anywhere, vmem, vmem],
        out_specs=anywhere,
        scratch_shapes=[
            pltpu.VMEM((gx, gy, bx * by, bz), f32),
            pltpu.VMEM((gx, gy, bx * by, bz), f32),
            pltpu.VMEM((nx, ny, bz), f32),
            pltpu.VMEM((nx + 2 * R, ny + 16, bz), f32),
            pltpu.VMEM((nx + 2 * R, ny + 16, bz), f32),
            pltpu.VMEM((nx, ny + 16, bz), f32),
            pltpu.VMEM((nx + 2 * R, ny, bz), f32),
            pltpu.VMEM((nx + 2 * R, ny, bz), f32),
            pltpu.VMEM((nx, ny, bz), f32),
            pltpu.VMEM((gx, gy, bx * by, bz), f32),
            pltpu.VMEM(edge, f32),
            pltpu.VMEM(edge, f32),
            dma((gx * gy,)), dma((gx, gy)),
            dma((2 * gx * gy,)), dma((gx, gy)),
            dma((gx,)), dma((gx,)),
            dma((DEGREE, gx, 2)), dma((DEGREE, gx, 2)),
            dma((gx * gy,)), dma((gx * gy,)),
            dma((3,)),
        ],
        compiler_params=pltpu.CompilerParams(
            collective_id=0, has_side_effects=True, vmem_limit_bytes=48 * 1024 * 1024
        ),
    )(
        orbitals.reshape(bands, bx * by, bz),
        potential.reshape(bx * by, bz),
        whi,
        wlo,
    )
    return out.reshape(bands, bx, by, bz)


def solution(mesh):
    sizes = tuple(mesh.shape[a] for a in ("gx", "gy", "gz"))
    return jax.shard_map(
        functools.partial(local, sizes),
        mesh=mesh,
        in_specs=(P(None, "gx", "gy", "gz"), P("gx", "gy", "gz")),
        out_specs=P(None, "gx", "gy", "gz"),
        check_vma=False,
    )
```

```python
import functools
import math

import jax
import jax.numpy as jnp
import numpy as np
from jax import lax
from jax.experimental import pallas as pl
from jax.experimental.pallas import tpu as pltpu
from jax.sharding import PartitionSpec as P

DEGREE = 2
VMEM_BYTES = 54_300_000
SECOND = (
    -5369.0 / 1800.0,
    12.0 / 7.0,
    -15.0 / 56.0,
    10.0 / 189.0,
    -1.0 / 112.0,
    2.0 / 1925.0,
    -1.0 / 16632.0,
)
FIRST = (6.0 / 7.0, -15.0 / 56.0, 5.0 / 63.0, -1.0 / 56.0, 3.0 / 385.0, -1.0 / 792.0)
METRIC = ((1.0, 0.25, 0.15), (0.25, 1.0, 0.2), (0.15, 0.2, 1.0))
CENTER = 10.5
HALF_WIDTH = 9.5
R = 6
Y0 = 8
MESH = pl.DeviceIdType.MESH


def halves(x):
    high = float(np.float32(x).astype(jnp.bfloat16))
    return high, float(np.float32(x - high).astype(jnp.bfloat16))


def bands_of(offset, part):
    out = []
    for table, sign in ((FIRST, -1.0), ([-0.5 * METRIC[2][2] * c for c in SECOND[1:]], 1.0)):
        acc = jnp.zeros(offset.shape, jnp.float32)
        for k in range(1, R + 1):
            value = halves(table[k - 1])[part]
            acc = jnp.where(offset == k, value, acc)
            acc = jnp.where(offset == -k, sign * value, acc)
        out.append(acc)
    return jnp.concatenate(out, axis=1).astype(jnp.bfloat16)


def z_matrices(bz, inner_ref, outer_ref):
    def index(shape, dim):
        return lax.broadcasted_iota(jnp.int32, shape, dim)

    square, edge = (bz, bz), (16, bz)
    offset = index(square, 0) - index(square, 1)
    e = index(edge, 0)
    beyond = jnp.where(e < 8, e - 8, e - 8 + bz) - index(edge, 1)
    high, edge_high = bands_of(offset, 0), bands_of(beyond, 0)
    inner_ref[pl.ds(0, bz), :] = high
    inner_ref[pl.ds(bz, bz), :] = high
    outer_ref[pl.ds(0, bz), :] = bands_of(offset, 1)
    outer_ref[pl.ds(bz, 16), :] = edge_high
    outer_ref[pl.ds(bz + 16, 16), :] = edge_high
    outer_ref[pl.ds(bz + 32, 16), :] = bands_of(beyond, 1)
    outer_ref[pl.ds(bz + 48, 80), :] = jnp.zeros((80, 2 * bz), jnp.bfloat16)


def kernel(
    gx, gy, gz, bx, by,
    orb, pot, out,
    inner_ref, outer_ref, vin, pin, p_ref, v0, v1, a_ref, c0, c1, s_ref, obuf, ebuf, hbuf,
    isend, irecv, psend, precv, qsend, qrecv, hsend, hrecv, osend, orecv, lsem,
):
    bz = orb.shape[-1]
    nx, ny = gx * bx, gy * by
    group = 8 // math.gcd(by, 8)
    rows = bx * ny
    padded_rows = ebuf.shape[-1]
    cx, cy, cz = lax.axis_index("gx"), lax.axis_index("gy"), lax.axis_index("gz")
    band = cx * gy + cy
    zl, zr = lax.rem(cz + gz - 1, gz), lax.rem(cz + 1, gz)
    odd = lax.rem(cx, 2)
    chip = cx - odd
    partner = chip + 1 - odd

    def across(d):
        ty, bit = cy, 1
        while bit <= d:
            if d & bit:
                ty = ty + bit - 2 * bit * lax.rem(lax.div(cy, bit), 2)
            bit *= 2
        return ty

    far_first = list(range(gy - 1, 0, -1))

    own_pot = pltpu.make_async_copy(pot, pin.at[cx, cy], lsem.at[1])
    own_pot.start()
    own_band = pltpu.make_async_copy(orb.at[:, band], vin.at[cx, cy], lsem.at[0])
    own_band.start()
    barrier = pltpu.get_barrier_semaphore()
    for dx in range(gx):
        for dy in range(gy):
            if dx or dy:
                pl.semaphore_signal(
                    barrier, inc=1,
                    device_id=(lax.rem(cx + dx, gx), lax.rem(cy + dy, gy), cz),
                    device_id_type=MESH,
                )
    for z in (zl, zr):
        pl.semaphore_signal(barrier, inc=1, device_id=(cx, cy, z), device_id_type=MESH)
    pl.semaphore_wait(barrier, gx * gy + 1)

    masks = []
    m = gy - 1
    while m:
        masks.append(m)
        m //= 2
    mates = [lax.rem(cx + 2 * i, gx) for i in range(1, gx // 2)]
    pot_out = []

    def send_pot(src, x, y, target):
        copy = pltpu.make_async_remote_copy(
            src, pin.at[x, y], psend.at[len(pot_out)], precv.at[x, y],
            device_id=target + (cz,), device_id_type=MESH,
        )
        copy.start()
        pot_out.append(copy)

    def wait_pot(x, y):
        pltpu.make_async_remote_copy(
            pot, pin.at[x, y], psend.at[0], precv.at[x, y],
            device_id=(partner, cy, cz), device_id_type=MESH,
        ).wait_recv()

    def share_pot():
        copies = []
        for i, x in enumerate([cx] + mates):
            copy = pltpu.make_async_remote_copy(
                pin.at[x], pin.at[x], qsend.at[i], qrecv.at[i],
                device_id=(partner, cy, cz), device_id_type=MESH,
            )
            copy.start()
            copies.append(copy)
        return copies

    bands_out = []

    def send_band(n, tx, ty):
        copy = pltpu.make_async_remote_copy(
            orb.at[:, tx * gy + ty], vin.at[cx, cy], isend.at[n], irecv.at[cx, cy],
            device_id=(tx, ty, cz), device_id_type=MESH,
        )
        copy.start()
        bands_out.append(copy)

    def send_group(g, pairs, ds):
        for d in ds:
            for i in pairs:
                if i or d:
                    n = (g * (gx // 2) + i) * gy + d
                    send_band(n, lax.rem(chip + 2 * i + g, gx), across(d))

    def wait_block(sx, own):
        for d in range(gy):
            sy = across(d)
            if own and d == 0:
                own_band.wait()
            else:
                pltpu.make_async_remote_copy(
                    orb.at[:, band], vin.at[sx, sy], isend.at[0], irecv.at[sx, sy],
                    device_id=(partner, cy, cz), device_id_type=MESH,
                ).wait_recv()

    def wrap_y(ref, x):
        ref[x, pl.ds(Y0 - R, R), :] = ref[x, pl.ds(Y0 + ny - R, R), :]
        ref[x, pl.ds(Y0 + ny, R), :] = ref[x, pl.ds(Y0, R), :]

    def wrap_x(ref, sx):
        @pl.when(sx == 0)
        def _():
            ref[pl.ds(nx + R, R)] = ref[pl.ds(R, R)]

        @pl.when(sx == gx - 1)
        def _():
            ref[pl.ds(0, R)] = ref[pl.ds(nx, R)]

    def pieces(sx, i):
        at = pl.multiple_of(i * group * by, 8)
        for sy in range(gy):
            got = vin[sx, sy, pl.ds(at, group * by), :]
            for j in range(group):
                yield sy, j, got[j * by : (j + 1) * by]

    def assemble(sx):
        @pl.loop(0, bx // group)
        def _(i):
            x = sx * bx + i * group + R
            for sy, j, piece in pieces(sx, i):
                v0[x + j, pl.ds(Y0 + sy * by, by), :] = piece
            for j in range(group):
                wrap_y(v0, x + j)
        wrap_x(v0, sx)

    def assemble_potential():
        for sx in range(gx):
            @pl.loop(0, bx)
            def _(i):
                for sy in range(gy):
                    p_ref[sx * bx + i, pl.ds(sy * by, by), :] = pin[sx, sy, i] + (
                        -1.5 * SECOND[0] - CENTER
                    )

    def send_edges(step, v, sx, t):
        vals = v[pl.ds(sx * bx + R, bx), pl.ds(Y0, ny), :].reshape(rows, bz)
        if padded_rows > rows:
            vals = jnp.concatenate([vals, jnp.zeros((padded_rows - rows, bz), jnp.float32)], axis=0)
        for i in range(padded_rows // 128):
            turned = vals[i * 128 : (i + 1) * 128].T
            ebuf[step, t, 0, :, pl.ds(i * 128, 128)] = turned[:8]
            ebuf[step, t, 1, :, pl.ds(i * 128, 128)] = turned[bz - 8 :]
        copies = []
        for side, z in ((0, zl), (1, zr)):
            copy = pltpu.make_async_remote_copy(
                ebuf.at[step, t, side], hbuf.at[step, t, 1 - side],
                hsend.at[step, t, side], hrecv.at[step, t, 1 - side],
                device_id=(cx, cy, z), device_id_type=MESH,
            )
            copy.start()
            copies.append(copy)
        return copies

    def y_pass(v, c_ref, sx):
        @pl.loop(0, bx)
        def _(i):
            x = sx * bx + i
            first = second = None
            for k in range(1, R + 1):
                up = v[x + R, pl.ds(Y0 + k, ny), :]
                down = v[x + R, pl.ds(Y0 - k, ny), :]
                f = (-METRIC[0][1] * FIRST[k - 1]) * (up - down)
                s = (-0.5 * METRIC[1][1] * SECOND[k]) * (up + down)
                first = f if first is None else first + f
                second = s if second is None else second + s
            c_ref[x + R] = first
            s_ref[x] = second

    def split(x):
        high = x.astype(jnp.bfloat16)
        return high, (x - high.astype(jnp.float32)).astype(jnp.bfloat16)

    def z_pass(step, v, c_ref, sx, t):
        vals = v[pl.ds(sx * bx + R, bx), pl.ds(Y0, ny), :].reshape(rows, bz)
        high, low = split(vals)
        sides = []
        for i in range(padded_rows // 128):
            edge = jnp.concatenate(
                [hbuf[step, t, side, :, pl.ds(i * 128, 128)] for side in (0, 1)], axis=0
            )
            eh, el = (e.astype(jnp.float32) for e in split(edge))
            block = jnp.concatenate([eh, el, eh, jnp.zeros((80, 128), jnp.float32)], axis=0)
            sides.append(block.T.astype(jnp.bfloat16))
        side = jnp.concatenate(sides, axis=0)[:rows]
        dot = functools.partial(jnp.dot, preferred_element_type=jnp.float32)
        got = dot(jnp.concatenate([high, low], axis=1), inner_ref[...])
        got = got + dot(jnp.concatenate([high, side], axis=1), outer_ref[...])
        a = got[:, :bz].reshape(bx, ny, bz)
        s_ref[pl.ds(sx * bx, bx)] += got[:, bz:].reshape(bx, ny, bz)
        c_ref[pl.ds(sx * bx + R, bx)] += (-METRIC[0][2]) * a
        a_ref[pl.ds(sx * bx, bx), pl.ds(Y0, ny), :] = a
        for i in range(bx):
            wrap_y(a_ref, sx * bx + i)
        wrap_x(c_ref, sx)

    def x_row(v, c_ref, x):
        total = s_ref[x] + p_ref[x] * v[x + R, pl.ds(Y0, ny), :]
        for k in range(1, R + 1):
            total = total + (-0.5 * METRIC[0][0] * SECOND[k]) * (
                v[x + R + k, pl.ds(Y0, ny), :] + v[x + R - k, pl.ds(Y0, ny), :]
            )
            total = total + FIRST[k - 1] * (c_ref[x + R + k] - c_ref[x + R - k])
            total = total + (-METRIC[1][2] * FIRST[k - 1]) * (
                a_ref[x, pl.ds(Y0 + k, ny), :] - a_ref[x, pl.ds(Y0 - k, ny), :]
            )
        return total

    def wait_all(copies):
        for copy in copies:
            copy.wait()

    block = [lax.rem(cx + gx + t - 2 * t * odd, gx) for t in range(gx)]
    second_edges = {}

    def first_x_pass(t):
        sx = block[t]

        @pl.loop(0, bx)
        def _(i):
            x = sx * bx + i
            v1[x + R, pl.ds(Y0, ny), :] = (1.0 / HALF_WIDTH) * x_row(v0, c0, x)
            wrap_y(v1, x + R)
        wrap_x(v1, sx)
        second_edges[t] = send_edges(1, v1, sx, t)
        y_pass(v1, c1, sx)

    far = list(range(gy - 1, gy // 2 - 1, -1))
    near = list(range(gy // 2 - 1, -1, -1))
    others = list(range(1, gx // 2))

    own_pot.wait()
    for d in masks:
        send_pot(pin.at[cx, cy], cx, cy, (cx, across(d)))
    for x in mates:
        send_pot(pin.at[cx, cy], cx, cy, (x, cy))
    send_band(0, partner, cy)
    send_group(0, [0], far)
    z_matrices(bz, inner_ref, outer_ref)
    reached = [0]
    for d in masks:
        wait_pot(cx, across(d))
    for x in mates:
        wait_pot(x, cy)
        for d in masks:
            send_pot(pin.at[cx, across(d)], cx, across(d), (x, cy))
    hops = []
    for k, m in enumerate(masks):
        if k:
            hops.append((m, [o for o in reached if o]))
        reached = reached + [o ^ m for o in reached]

    def forward(x, hop):
        m, offsets = hop
        for o in offsets:
            send_pot(pin.at[x, across(o)], x, across(o), (cx, across(m)))

    def arrive(x, hop):
        m, offsets = hop
        for o in offsets:
            wait_pot(x, across(o ^ m))

    for hop in hops[:1]:
        forward(cx, hop)
    send_group(0, others, far + near)
    for k, hop in enumerate(hops):
        if k:
            forward(cx, hop)
        arrive(cx, hop)
    for x in mates:
        for d in masks:
            wait_pot(x, across(d))
        for hop in hops[:1]:
            forward(x, hop)
    send_group(0, [0], near)
    for k, hop in enumerate(hops):
        for x in mates:
            if k:
                forward(x, hop)
            arrive(x, hop)
    sharing = share_pot()
    send_group(1, [0] + others, near + far)
    first_edges = []
    for t in range(gx):
        wait_block(block[t], t == 0)
        assemble(block[t])
        first_edges.append(send_edges(0, v0, block[t], t))
        if t >= 1:
            y_pass(v0, c0, block[t - 1])
    y_pass(v0, c0, block[gx - 1])
    wait_all(sharing)
    assemble_potential()
    for t in range(gx - 1):
        wait_all(first_edges[t])
        z_pass(0, v0, c0, block[t], t)
    for t in range(1, gx - 2):
        first_x_pass(t)
    wait_all(first_edges[gx - 1])
    z_pass(0, v0, c0, block[gx - 1], gx - 1)
    late = [gx - 2, gx - 1, 0]
    for t in late:
        first_x_pass(t)

    outgoing = []

    def last_x_pass(t):
        sx = block[t]

        @pl.loop(0, bx // group)
        def _(i):
            got = []
            for j in range(group):
                x = sx * bx + i * group + j
                got.append(
                    (2.0 / HALF_WIDTH) * x_row(v1, c1, x) - v0[x + R, pl.ds(Y0, ny), :]
                )
            at = pl.multiple_of(i * group * by, 8)
            for sy in range(gy):
                obuf[sx, sy, pl.ds(at, group * by), :] = jnp.concatenate(
                    [g[sy * by : (sy + 1) * by] for g in got], axis=0
                )

        for dy in far_first + [0]:
            ty = across(dy)
            n = t * gy + dy
            if n == 0:
                copy = pltpu.make_async_copy(obuf.at[sx, ty], out.at[:, band], lsem.at[2])
            else:
                copy = pltpu.make_async_remote_copy(
                    obuf.at[sx, ty], out.at[:, band], osend.at[n], orecv.at[n],
                    device_id=(sx, ty, cz), device_id_type=MESH,
                )
            copy.start()
            outgoing.append(copy)

    ready = list(range(1, gx - 2)) + late
    done = []
    for t in ready:
        wait_all(second_edges[t])
        z_pass(1, v1, c1, block[t], t)
        done.append(t)
        for u in range(gx):
            near = {u, (u + 1) % gx, (u - 1) % gx}
            if near <= set(done) and t in near:
                last_x_pass(u)
    wait_all(outgoing)
    for copy in bands_out + pot_out:
        copy.wait_send()


def local(sizes, orbitals, potential):
    gx, gy, gz = sizes
    bands, bx, by, bz = orbitals.shape
    nx, ny = gx * bx, gy * by
    assert bands == gx * gy and gz > 1 and gx >= 4 and gx & (gx - 1) == 0
    f32 = jnp.float32
    anywhere = pl.BlockSpec(memory_space=pl.ANY)
    dma = pltpu.SemaphoreType.DMA
    edge = (DEGREE, gx, 2, 8, (bx * ny + 127) // 128 * 128)
    out = pl.pallas_call(
        functools.partial(kernel, gx, gy, gz, bx, by),
        out_shape=jax.ShapeDtypeStruct((bx * by, bands, bz), f32),
        in_specs=[anywhere] * 2,
        out_specs=anywhere,
        scratch_shapes=[
            pltpu.VMEM((2 * bz, 2 * bz), jnp.bfloat16),
            pltpu.VMEM((bz + 128, 2 * bz), jnp.bfloat16),
            pltpu.VMEM((gx, gy, bx * by, bz), f32),
            pltpu.VMEM((gx, gy, bx, by, bz), f32),
            pltpu.VMEM((nx, ny, bz), f32),
            pltpu.VMEM((nx + 2 * R, ny + 16, bz), f32),
            pltpu.VMEM((nx + 2 * R, ny + 16, bz), f32),
            pltpu.VMEM((nx, ny + 16, bz), f32),
            pltpu.VMEM((nx + 2 * R, ny, bz), f32),
            pltpu.VMEM((nx + 2 * R, ny, bz), f32),
            pltpu.VMEM((nx, ny, bz), f32),
            pltpu.VMEM((gx, gy, bx * by, bz), f32),
            pltpu.VMEM(edge, f32),
            pltpu.VMEM(edge, f32),
            dma((gx * gy,)), dma((gx, gy)),
            dma((2 * gx * gy,)), dma((gx, gy)),
            dma((gx,)), dma((gx,)),
            dma((DEGREE, gx, 2)), dma((DEGREE, gx, 2)),
            dma((gx * gy,)), dma((gx * gy,)),
            dma((3,)),
        ],
        compiler_params=pltpu.CompilerParams(
            collective_id=0, has_side_effects=True, vmem_limit_bytes=VMEM_BYTES
        ),
    )(
        orbitals.transpose(1, 2, 0, 3).reshape(bx * by, bands, bz),
        potential,
    )
    return out.reshape(bx, by, bands, bz).transpose(2, 0, 1, 3)


def solution(mesh):
    sizes = tuple(mesh.shape[a] for a in ("gx", "gy", "gz"))
    return jax.shard_map(
        functools.partial(local, sizes),
        mesh=mesh,
        in_specs=(P(None, "gx", "gy", "gz"), P("gx", "gy", "gz")),
        out_specs=P(None, "gx", "gy", "gz"),
        check_vma=False,
    )
```

```python
import functools
import math

import jax
import jax.numpy as jnp
import numpy as np
from jax import lax
from jax.experimental import pallas as pl
from jax.experimental.pallas import tpu as pltpu
from jax.sharding import PartitionSpec as P

DEGREE = 2
SECOND = (
    -5369.0 / 1800.0,
    12.0 / 7.0,
    -15.0 / 56.0,
    10.0 / 189.0,
    -1.0 / 112.0,
    2.0 / 1925.0,
    -1.0 / 16632.0,
)
FIRST = (6.0 / 7.0, -15.0 / 56.0, 5.0 / 63.0, -1.0 / 56.0, 3.0 / 385.0, -1.0 / 792.0)
METRIC = ((1.0, 0.25, 0.15), (0.25, 1.0, 0.2), (0.15, 0.2, 1.0))
CENTER = 10.5
HALF_WIDTH = 9.5
R = 6
Y0 = 8
MESH = pl.DeviceIdType.MESH


def halves(x):
    high = float(np.float32(x).astype(jnp.bfloat16))
    return high, float(np.float32(x - high).astype(jnp.bfloat16))


def bands_of(offset, part):
    out = []
    cross = [-METRIC[1][2] * c for c in FIRST]
    for table, sign in ((cross, -1.0), ([-0.5 * METRIC[2][2] * c for c in SECOND[1:]], 1.0)):
        acc = jnp.zeros(offset.shape, jnp.float32)
        for k in range(1, R + 1):
            value = halves(table[k - 1])[part]
            acc = jnp.where(offset == k, value, acc)
            acc = jnp.where(offset == -k, sign * value, acc)
        out.append(acc)
    return jnp.concatenate(out, axis=1).astype(jnp.bfloat16)


def z_matrix(bz, w_ref):
    def index(shape, dim):
        return lax.broadcasted_iota(jnp.int32, shape, dim)

    square, edge = (bz, bz), (16, bz)
    offset = index(square, 0) - index(square, 1)
    e = index(edge, 0)
    beyond = jnp.where(e < 8, e - 8, e - 8 + bz) - index(edge, 1)
    high, edge_high = bands_of(offset, 0), bands_of(beyond, 0)
    parts = [high, high, bands_of(offset, 1), edge_high, edge_high, bands_of(beyond, 1)]
    parts.append(jnp.zeros((80, 2 * bz), jnp.bfloat16))
    at = 0
    for part in parts:
        w_ref[pl.ds(at, part.shape[0]), :] = part
        at += part.shape[0]


def kernel(
    gx, gy, gz, bx, by,
    orb, pot, out,
    w_ref, vin, pin, p_ref, v0, v1, a_ref, c0, c1, s_ref, obuf, ebuf, hbuf,
    isend, irecv, psend, precv, qsend, qrecv, hsend, hrecv, osend, orecv, lsem,
):
    bz = orb.shape[-1]
    nx, ny = gx * bx, gy * by
    group = 8 // math.gcd(by, 8)
    rows = bx * ny
    padded_rows = ebuf.shape[-1]
    cx, cy, cz = lax.axis_index("gx"), lax.axis_index("gy"), lax.axis_index("gz")
    band = cx * gy + cy
    zl, zr = lax.rem(cz + gz - 1, gz), lax.rem(cz + 1, gz)
    odd = lax.rem(cx, 2)
    chip = cx - odd
    partner = chip + 1 - odd

    def across(d):
        ty, bit = cy, 1
        while bit <= d:
            if d & bit:
                ty = ty + bit - 2 * bit * lax.rem(lax.div(cy, bit), 2)
            bit *= 2
        return ty

    far_first = list(range(gy - 1, 0, -1))

    own_pot = pltpu.make_async_copy(pot, pin.at[cx, cy], lsem.at[1])
    own_pot.start()
    own_band = pltpu.make_async_copy(orb.at[:, band], vin.at[cx, cy], lsem.at[0])
    own_band.start()
    barrier = pltpu.get_barrier_semaphore()
    for dx in range(gx):
        for dy in range(gy):
            if dx or dy:
                pl.semaphore_signal(
                    barrier, inc=1,
                    device_id=(lax.rem(cx + dx, gx), lax.rem(cy + dy, gy), cz),
                    device_id_type=MESH,
                )
    for z in (zl, zr):
        pl.semaphore_signal(barrier, inc=1, device_id=(cx, cy, z), device_id_type=MESH)
    pl.semaphore_wait(barrier, gx * gy + 1)

    masks = []
    m = gy - 1
    while m:
        masks.append(m)
        m //= 2
    mates = [lax.rem(cx + 2 * i, gx) for i in range(1, gx // 2)]
    pot_out = []

    def send_pot(src, x, y, target):
        copy = pltpu.make_async_remote_copy(
            src, pin.at[x, y], psend.at[len(pot_out)], precv.at[x, y],
            device_id=target + (cz,), device_id_type=MESH,
        )
        copy.start()
        pot_out.append(copy)

    def wait_pot(x, y):
        pltpu.make_async_remote_copy(
            pot, pin.at[x, y], psend.at[0], precv.at[x, y],
            device_id=(partner, cy, cz), device_id_type=MESH,
        ).wait_recv()

    def share_pot():
        copies = []
        for i, x in enumerate([cx] + mates):
            copy = pltpu.make_async_remote_copy(
                pin.at[x], pin.at[x], qsend.at[i], qrecv.at[i],
                device_id=(partner, cy, cz), device_id_type=MESH,
            )
            copy.start()
            copies.append(copy)
        return copies

    bands_out = []

    def send_band(n, tx, ty):
        copy = pltpu.make_async_remote_copy(
            orb.at[:, tx * gy + ty], vin.at[cx, cy], isend.at[n], irecv.at[cx, cy],
            device_id=(tx, ty, cz), device_id_type=MESH,
        )
        copy.start()
        bands_out.append(copy)

    def send_group(g, pairs, ds):
        for d in ds:
            for i in pairs:
                if i or d:
                    n = (g * (gx // 2) + i) * gy + d
                    send_band(n, lax.rem(chip + 2 * i + g, gx), across(d))

    def wait_block(sx, own):
        for d in range(gy):
            sy = across(d)
            if own and d == 0:
                own_band.wait()
            else:
                pltpu.make_async_remote_copy(
                    orb.at[:, band], vin.at[sx, sy], isend.at[0], irecv.at[sx, sy],
                    device_id=(partner, cy, cz), device_id_type=MESH,
                ).wait_recv()

    def wrap_y(ref, x):
        ref[x, pl.ds(Y0 - R, R), :] = ref[x, pl.ds(Y0 + ny - R, R), :]
        ref[x, pl.ds(Y0 + ny, R), :] = ref[x, pl.ds(Y0, R), :]

    def wrap_x(ref, sx):
        @pl.when(sx == 0)
        def _():
            ref[pl.ds(nx + R, R)] = ref[pl.ds(R, R)]

        @pl.when(sx == gx - 1)
        def _():
            ref[pl.ds(0, R)] = ref[pl.ds(nx, R)]

    def pieces(sx, i):
        at = pl.multiple_of(i * group * by, 8)
        for sy in range(gy):
            got = vin[sx, sy, pl.ds(at, group * by), :]
            for j in range(group):
                yield sy, j, got[j * by : (j + 1) * by]

    def assemble(sx):
        @pl.loop(0, bx // group)
        def _(i):
            x = sx * bx + i * group + R
            for sy, j, piece in pieces(sx, i):
                v0[x + j, pl.ds(Y0 + sy * by, by), :] = piece
            for j in range(group):
                wrap_y(v0, x + j)
        wrap_x(v0, sx)

    def assemble_potential():
        for sx in range(gx):
            @pl.loop(0, bx)
            def _(i):
                for sy in range(gy):
                    p_ref[sx * bx + i, pl.ds(sy * by, by), :] = pin[sx, sy, i] + (
                        -1.5 * SECOND[0] - CENTER
                    )

    def edge_copies(step, t):
        return [
            pltpu.make_async_remote_copy(
                ebuf.at[step, t, side], hbuf.at[step, t, 1 - side],
                hsend.at[step, t, side], hrecv.at[step, t, 1 - side],
                device_id=(cx, cy, z), device_id_type=MESH,
            )
            for side, z in ((0, zl), (1, zr))
        ]

    def send_edges(step, v, sx, t):
        vals = v[pl.ds(sx * bx + R, bx), pl.ds(Y0, ny), :].reshape(rows, bz)
        if padded_rows > rows:
            vals = jnp.concatenate([vals, jnp.zeros((padded_rows - rows, bz), jnp.float32)], axis=0)
        for i in range(padded_rows // 128):
            turned = vals[i * 128 : (i + 1) * 128].T
            ebuf[step, t, 0, :, pl.ds(i * 128, 128)] = turned[:8]
            ebuf[step, t, 1, :, pl.ds(i * 128, 128)] = turned[bz - 8 :]
        for copy in edge_copies(step, t):
            copy.start()

    def y_pass(v, c_ref, sx):
        @pl.loop(0, bx)
        def _(i):
            x = sx * bx + i
            first = second = None
            for k in range(1, R + 1):
                up = v[x + R, pl.ds(Y0 + k, ny), :]
                down = v[x + R, pl.ds(Y0 - k, ny), :]
                f = (-METRIC[0][1] * FIRST[k - 1]) * (up - down)
                s = (-0.5 * METRIC[1][1] * SECOND[k]) * (up + down)
                first = f if first is None else first + f
                second = s if second is None else second + s
            c_ref[x + R] = first
            s_ref[x] = second

    def split(x):
        high = x.astype(jnp.bfloat16)
        return high, (x - high.astype(jnp.float32)).astype(jnp.bfloat16)

    def z_pass(step, v, c_ref, sx, t):
        vals = v[pl.ds(sx * bx + R, bx), pl.ds(Y0, ny), :].reshape(rows, bz)
        high, low = split(vals)
        sides = []
        for i in range(padded_rows // 128):
            edge = jnp.concatenate(
                [hbuf[step, t, side, :, pl.ds(i * 128, 128)] for side in (0, 1)], axis=0
            )
            eh, el = (e.astype(jnp.float32) for e in split(edge))
            block = jnp.concatenate([eh, el, eh, jnp.zeros((80, 128), jnp.float32)], axis=0)
            sides.append(block.T.astype(jnp.bfloat16))
        side = jnp.concatenate(sides, axis=0)[:rows]
        got = jnp.dot(
            jnp.concatenate([high, low, high, side], axis=1), w_ref[...],
            preferred_element_type=jnp.float32,
        )
        a = got[:, :bz].reshape(bx, ny, bz)
        s_ref[pl.ds(sx * bx, bx)] += got[:, bz:].reshape(bx, ny, bz)
        c_ref[pl.ds(sx * bx + R, bx)] += (METRIC[0][2] / METRIC[1][2]) * a
        a_ref[pl.ds(sx * bx, bx), pl.ds(Y0, ny), :] = a
        for i in range(bx):
            wrap_y(a_ref, sx * bx + i)
        wrap_x(c_ref, sx)

    many = 4 if bx % 4 == 0 and 4 % group == 0 else group
    tall = math.gcd(ny, 8)

    def x_rows(v, c_ref, x, y):
        vs = [v[x + i, pl.ds(Y0 + y, tall), :] for i in range(many + 2 * R)]
        cs = [c_ref[x + i, pl.ds(y, tall), :] for i in range(many + 2 * R)]
        totals = []
        for g in range(many):
            mid = g + R
            total = s_ref[x + g, pl.ds(y, tall), :] + p_ref[x + g, pl.ds(y, tall), :] * vs[mid]
            for k in range(1, R + 1):
                second = vs[mid + k] + vs[mid - k]
                first = (cs[mid + k] - cs[mid - k]) + (
                    a_ref[x + g, pl.ds(Y0 + y + k, tall), :]
                    - a_ref[x + g, pl.ds(Y0 + y - k, tall), :]
                )
                total = total + (-0.5 * METRIC[0][0] * SECOND[k]) * second
                total = total + FIRST[k - 1] * first
            totals.append(total)
        return totals

    def wait_all(copies):
        for copy in copies:
            copy.wait()

    block = [lax.rem(cx + gx + t - 2 * t * odd, gx) for t in range(gx)]

    def first_x_pass(t):
        sx = block[t]

        @pl.loop(0, bx // many)
        def _(i):
            x = sx * bx + i * many
            for y in range(0, ny, tall):
                for g, total in enumerate(x_rows(v0, c0, x, y)):
                    v1[x + g + R, pl.ds(Y0 + y, tall), :] = (1.0 / HALF_WIDTH) * total
            for g in range(many):
                wrap_y(v1, x + g + R)
        wrap_x(v1, sx)
        send_edges(1, v1, sx, t)
        y_pass(v1, c1, sx)

    far = list(range(gy // 2, gy))
    near = list(range(gy // 2))
    others = list(range(1, gx // 2))

    own_pot.wait()
    for d in masks:
        send_pot(pin.at[cx, cy], cx, cy, (cx, across(d)))
    for x in mates:
        send_pot(pin.at[cx, cy], cx, cy, (x, cy))
    send_band(0, partner, cy)
    send_group(0, [0], near + far)
    z_matrix(bz, w_ref)
    reached = [0]
    for d in masks:
        wait_pot(cx, across(d))
    for x in mates:
        wait_pot(x, cy)
        for d in masks:
            send_pot(pin.at[cx, across(d)], cx, across(d), (x, cy))
    hops = []
    for k, m in enumerate(masks):
        if k:
            hops.append((m, [o for o in reached if o]))
        reached = reached + [o ^ m for o in reached]

    def forward(hop):
        m, offsets = hop
        for o in offsets:
            for x in [cx] + mates:
                send_pot(pin.at[cx, across(o)], cx, across(o), (x, across(m)))

    def arrive(hop):
        m, offsets = hop
        for o in offsets:
            for x in [cx] + mates:
                wait_pot(x, across(o ^ m))

    for hop in hops[:1]:
        forward(hop)
    first_group = [len(bands_out)]
    send_group(0, others, near + far)
    first_group.append(len(bands_out))

    def enter(t):
        wait_block(block[t], t == 0)
        assemble(block[t])
        send_edges(0, v0, block[t], t)
        y_pass(v0, c0, block[t])

    def enter_chip():
        enter(0)
        enter(1)

    pl.when(odd == 0)(enter_chip)
    for k, hop in enumerate(hops):
        if k:
            forward(hop)
        arrive(hop)
    for x in mates:
        for d in masks:
            wait_pot(x, across(d))
    sharing = share_pot()
    for copy in bands_out[slice(*first_group)]:
        copy.wait_send()
    del bands_out[slice(*first_group)]
    send_group(1, [0] + others, near + far)
    pl.when(odd == 1)(enter_chip)
    for t in (0, 1):
        wait_all(edge_copies(0, t))
        z_pass(0, v0, c0, block[t], t)
    for t in range(2, gx):
        enter(t)
    wait_all(sharing)
    assemble_potential()
    for t in range(2, gx - 1):
        wait_all(edge_copies(0, t))
        z_pass(0, v0, c0, block[t], t)
    for t in range(1, gx - 2):
        first_x_pass(t)
    wait_all(edge_copies(0, gx - 1))
    z_pass(0, v0, c0, block[gx - 1], gx - 1)
    for t in (gx - 2, gx - 1, 0):
        first_x_pass(t)

    outgoing = []

    def last_x_pass(t):
        sx = block[t]

        @pl.loop(0, bx // many)
        def _(i):
            x = sx * bx + i * many
            at = pl.multiple_of(i * many * by, 8)
            for y in range(0, ny, tall):
                for g, total in enumerate(x_rows(v1, c1, x, y)):
                    got = (2.0 / HALF_WIDTH) * total - v0[x + g + R, pl.ds(Y0 + y, tall), :]
                    low = y
                    while low < y + tall:
                        sy = low // by
                        high = min(y + tall, (sy + 1) * by)
                        obuf[sx, sy, pl.ds(at + g * by + low - sy * by, high - low), :] = got[
                            low - y : high - y
                        ]
                        low = high

        for dy in range(gy):
            ty = across(dy)
            n = t * gy + dy
            if n == 0:
                copy = pltpu.make_async_copy(obuf.at[sx, ty], out.at[:, band], lsem.at[2])
            else:
                copy = pltpu.make_async_remote_copy(
                    obuf.at[sx, ty], out.at[:, band], osend.at[n], orecv.at[n],
                    device_id=(sx, ty, cz), device_id_type=MESH,
                )
            copy.start()
            outgoing.append(copy)

    done = []
    for t in list(range(1, gx)) + [0]:
        wait_all(edge_copies(1, t))
        z_pass(1, v1, c1, block[t], t)
        done.append(t)
        for u in range(gx):
            near = {u, (u + 1) % gx, (u - 1) % gx}
            if near <= set(done) and t in near:
                last_x_pass(u)
    wait_all(outgoing)
    for copy in bands_out + pot_out:
        copy.wait_send()


def local(sizes, orbitals, potential):
    gx, gy, gz = sizes
    bands, bx, by, bz = orbitals.shape
    nx, ny = gx * bx, gy * by
    assert bands == gx * gy and gz > 1 and gx >= 4 and gx & (gx - 1) == 0
    f32 = jnp.float32
    anywhere = pl.BlockSpec(memory_space=pl.ANY)
    dma = pltpu.SemaphoreType.DMA
    edge = (DEGREE, gx, 2, 8, (bx * ny + 127) // 128 * 128)
    out = pl.pallas_call(
        functools.partial(kernel, gx, gy, gz, bx, by),
        out_shape=jax.ShapeDtypeStruct((bx * by, bands, bz), f32),
        in_specs=[anywhere] * 2,
        out_specs=anywhere,
        scratch_shapes=[
            pltpu.VMEM((3 * bz + 128, 2 * bz), jnp.bfloat16),
            pltpu.VMEM((gx, gy, bx * by, bz), f32),
            pltpu.VMEM((gx, gy, bx, by, bz), f32),
            pltpu.VMEM((nx, ny, bz), f32),
            pltpu.VMEM((nx + 2 * R, ny + 16, bz), f32),
            pltpu.VMEM((nx + 2 * R, ny + 16, bz), f32),
            pltpu.VMEM((nx, ny + 16, bz), f32),
            pltpu.VMEM((nx + 2 * R, ny, bz), f32),
            pltpu.VMEM((nx + 2 * R, ny, bz), f32),
            pltpu.VMEM((nx, ny, bz), f32),
            pltpu.VMEM((gx, gy, bx * by, bz), f32),
            pltpu.VMEM(edge, f32),
            pltpu.VMEM(edge, f32),
            dma((gx * gy,)), dma((gx, gy)),
            dma((2 * gx * gy,)), dma((gx, gy)),
            dma((gx,)), dma((gx,)),
            dma((DEGREE, gx, 2)), dma((DEGREE, gx, 2)),
            dma((gx * gy,)), dma((gx * gy,)),
            dma((3,)),
        ],
        compiler_params=pltpu.CompilerParams(
            collective_id=0, has_side_effects=True, vmem_limit_bytes=48 * 1024 * 1024
        ),
    )(
        pltpu.with_memory_space_constraint(
            orbitals.transpose(1, 2, 0, 3).reshape(bx * by, bands, bz), pltpu.HBM
        ),
        pltpu.with_memory_space_constraint(potential, pltpu.HBM),
    )
    return out.reshape(bx, by, bands, bz).transpose(2, 0, 1, 3)


def solution(mesh):
    sizes = tuple(mesh.shape[a] for a in ("gx", "gy", "gz"))
    return jax.shard_map(
        functools.partial(local, sizes),
        mesh=mesh,
        in_specs=(P(None, "gx", "gy", "gz"), P("gx", "gy", "gz")),
        out_specs=P(None, "gx", "gy", "gz"),
        check_vma=False,
    )
```

```python
import functools
import math

import jax
import jax.numpy as jnp
import numpy as np
from jax import lax
from jax.experimental import pallas as pl
from jax.experimental.pallas import tpu as pltpu
from jax.sharding import PartitionSpec as P

DEGREE = 2
SECOND = (
    -5369.0 / 1800.0,
    12.0 / 7.0,
    -15.0 / 56.0,
    10.0 / 189.0,
    -1.0 / 112.0,
    2.0 / 1925.0,
    -1.0 / 16632.0,
)
FIRST = (6.0 / 7.0, -15.0 / 56.0, 5.0 / 63.0, -1.0 / 56.0, 3.0 / 385.0, -1.0 / 792.0)
METRIC = ((1.0, 0.25, 0.15), (0.25, 1.0, 0.2), (0.15, 0.2, 1.0))
CENTER = 10.5
HALF_WIDTH = 9.5
R = 6
Y0 = 8
MESH = pl.DeviceIdType.MESH


def halves(x):
    high = float(np.float32(x).astype(jnp.bfloat16))
    return high, float(np.float32(x - high).astype(jnp.bfloat16))


def bands_of(offset, part):
    out = []
    cross = [-METRIC[1][2] * c for c in FIRST]
    for table, sign in ((cross, -1.0), ([-0.5 * METRIC[2][2] * c for c in SECOND[1:]], 1.0)):
        acc = jnp.zeros(offset.shape, jnp.float32)
        for k in range(1, R + 1):
            value = halves(table[k - 1])[part]
            acc = jnp.where(offset == k, value, acc)
            acc = jnp.where(offset == -k, sign * value, acc)
        out.append(acc)
    return jnp.concatenate(out, axis=1).astype(jnp.bfloat16)


def z_matrix(bz, w_ref):
    def index(shape, dim):
        return lax.broadcasted_iota(jnp.int32, shape, dim)

    square, edge = (bz, bz), (16, bz)
    offset = index(square, 0) - index(square, 1)
    e = index(edge, 0)
    beyond = jnp.where(e < 8, e - 8, e - 8 + bz) - index(edge, 1)
    high, edge_high = bands_of(offset, 0), bands_of(beyond, 0)
    parts = [high, high, bands_of(offset, 1), edge_high, edge_high, bands_of(beyond, 1)]
    parts.append(jnp.zeros((80, 2 * bz), jnp.bfloat16))
    at = 0
    for part in parts:
        w_ref[pl.ds(at, part.shape[0]), :] = part
        at += part.shape[0]


def kernel(
    gx, gy, gz, bx, by,
    orb, pot, out,
    w_ref, vin, pin, p_ref, v0, v1, a_ref, c0, c1, s_ref, obuf, ebuf, hbuf,
    isend, irecv, psend, precv, qsend, qrecv, hsend, hrecv, osend, orecv, lsem,
):
    bz = orb.shape[-1]
    nx, ny = gx * bx, gy * by
    group = 8 // math.gcd(by, 8)
    rows = bx * ny
    padded_rows = ebuf.shape[-1]
    cx, cy, cz = lax.axis_index("gx"), lax.axis_index("gy"), lax.axis_index("gz")
    band = cx * gy + cy
    zl, zr = lax.rem(cz + gz - 1, gz), lax.rem(cz + 1, gz)
    odd = lax.rem(cx, 2)
    chip = cx - odd
    partner = chip + 1 - odd

    def across(d):
        ty, bit = cy, 1
        while bit <= d:
            if d & bit:
                ty = ty + bit - 2 * bit * lax.rem(lax.div(cy, bit), 2)
            bit *= 2
        return ty

    far_first = list(range(gy - 1, 0, -1))

    own_pot = pltpu.make_async_copy(pot, pin.at[cx, cy], lsem.at[0])
    own_pot.start()
    own_band = pltpu.make_async_copy(orb.at[:, band], vin.at[band], irecv.at[cx])
    own_band.start()
    barrier = pltpu.get_barrier_semaphore()
    for dx in range(gx):
        for dy in range(gy):
            if dx or dy:
                pl.semaphore_signal(
                    barrier, inc=1,
                    device_id=(lax.rem(cx + dx, gx), lax.rem(cy + dy, gy), cz),
                    device_id_type=MESH,
                )
    for z in (zl, zr):
        pl.semaphore_signal(barrier, inc=1, device_id=(cx, cy, z), device_id_type=MESH)
    pl.semaphore_wait(barrier, gx * gy + 1)

    masks = []
    m = gy - 1
    while m:
        masks.append(m)
        m //= 2
    mates = [lax.rem(cx + 2 * i, gx) for i in range(1, gx // 2)]
    pot_out = []

    def send_pot(y, target):
        i = len(pot_out)
        copy = pltpu.make_async_remote_copy(
            pin.at[cx, y], pin.at[cx, y], psend.at[i], precv.at[i],
            device_id=target + (cz,), device_id_type=MESH,
        )
        copy.start()
        pot_out.append(copy)
        return i

    def wait_pot(i):
        pot_out[i].wait_recv()

    def share_pot():
        copies = []
        for i, x in enumerate([cx] + mates):
            copy = pltpu.make_async_remote_copy(
                pin.at[x], pin.at[x], qsend.at[i], qrecv.at[i],
                device_id=(partner, cy, cz), device_id_type=MESH,
            )
            copy.start()
            copies.append(copy)
        return copies

    def meet(src, dst, send, recv):
        return pltpu.make_async_remote_copy(
            src, dst, send, recv, device_id=(partner, cy, cz), device_id_type=MESH
        )

    def send_band(tx, ty):
        pltpu.make_async_remote_copy(
            orb.at[:, tx * gy + ty], vin.at[band], isend.at[0], irecv.at[cx],
            device_id=(tx, ty, cz), device_id_type=MESH,
        ).start()

    def send_group(g, pairs, ds):
        for d in ds:
            for i in pairs:
                if i or d:
                    send_band(lax.rem(chip + 2 * i + g, gx), across(d))

    def wait_block(sx):
        blocks = vin.at[pl.ds(sx * gy, gy)]
        meet(blocks, blocks, isend.at[0], irecv.at[sx]).wait_recv()

    def wrap_y(ref, x):
        ref[x, pl.ds(Y0 - R, R), :] = ref[x, pl.ds(Y0 + ny - R, R), :]
        ref[x, pl.ds(Y0 + ny, R), :] = ref[x, pl.ds(Y0, R), :]

    def wrap_x(ref, sx):
        @pl.when(sx == 0)
        def _():
            ref[pl.ds(nx + R, R)] = ref[pl.ds(R, R)]

        @pl.when(sx == gx - 1)
        def _():
            ref[pl.ds(0, R)] = ref[pl.ds(nx, R)]

    def pieces(sx, i):
        at = pl.multiple_of(i * group * by, 8)
        for sy in range(gy):
            got = vin[sx * gy + sy, pl.ds(at, group * by), :]
            for j in range(group):
                yield sy, j, got[j * by : (j + 1) * by]

    def assemble(sx):
        @pl.loop(0, bx // group)
        def _(i):
            x = sx * bx + i * group + R
            for sy, j, piece in pieces(sx, i):
                v0[x + j, pl.ds(Y0 + sy * by, by), :] = piece
            for j in range(group):
                wrap_y(v0, x + j)
        wrap_x(v0, sx)

    def assemble_potential():
        for sx in range(gx):
            @pl.loop(0, bx)
            def _(i):
                for sy in range(gy):
                    p_ref[sx * bx + i, pl.ds(sy * by, by), :] = pin[sx, sy, i] + (
                        -1.5 * SECOND[0] - CENTER
                    )

    def edge_wait(step, t):
        meet(ebuf.at[step, t], hbuf.at[step, t], hsend.at[0], hrecv.at[step, t]).wait_recv()

    def edge_copies(step, t):
        return [
            pltpu.make_async_remote_copy(
                ebuf.at[step, t, side], hbuf.at[step, t, 1 - side],
                hsend.at[0], hrecv.at[step, t],
                device_id=(cx, cy, z), device_id_type=MESH,
            )
            for side, z in ((0, zl), (1, zr))
        ]

    def send_edges(step, v, sx, t):
        vals = v[pl.ds(sx * bx + R, bx), pl.ds(Y0, ny), :].reshape(rows, bz)
        if padded_rows > rows:
            vals = jnp.concatenate([vals, jnp.zeros((padded_rows - rows, bz), jnp.float32)], axis=0)
        for i in range(padded_rows // 128):
            turned = vals[i * 128 : (i + 1) * 128].T
            ebuf[step, t, 0, :, pl.ds(i * 128, 128)] = turned[:8]
            ebuf[step, t, 1, :, pl.ds(i * 128, 128)] = turned[bz - 8 :]
        for copy in edge_copies(step, t):
            copy.start()

    def y_pass(v, c_ref, sx):
        @pl.loop(0, bx)
        def _(i):
            x = sx * bx + i
            first = second = None
            for k in range(1, R + 1):
                up = v[x + R, pl.ds(Y0 + k, ny), :]
                down = v[x + R, pl.ds(Y0 - k, ny), :]
                f = (-METRIC[0][1] * FIRST[k - 1]) * (up - down)
                s = (-0.5 * METRIC[1][1] * SECOND[k]) * (up + down)
                first = f if first is None else first + f
                second = s if second is None else second + s
            c_ref[x + R] = first
            s_ref[x] = second

    def split(x):
        high = x.astype(jnp.bfloat16)
        return high, (x - high.astype(jnp.float32)).astype(jnp.bfloat16)

    def z_pass(step, v, c_ref, sx, t):
        vals = v[pl.ds(sx * bx + R, bx), pl.ds(Y0, ny), :].reshape(rows, bz)
        high, low = split(vals)
        sides = []
        for i in range(padded_rows // 128):
            edge = jnp.concatenate(
                [hbuf[step, t, side, :, pl.ds(i * 128, 128)] for side in (0, 1)], axis=0
            )
            eh, el = (e.astype(jnp.float32) for e in split(edge))
            block = jnp.concatenate([eh, el, eh, jnp.zeros((80, 128), jnp.float32)], axis=0)
            sides.append(block.T.astype(jnp.bfloat16))
        side = jnp.concatenate(sides, axis=0)[:rows]
        got = jnp.dot(
            jnp.concatenate([high, low, high, side], axis=1), w_ref[...],
            preferred_element_type=jnp.float32,
        )
        a = got[:, :bz].reshape(bx, ny, bz)
        s_ref[pl.ds(sx * bx, bx)] += got[:, bz:].reshape(bx, ny, bz)
        c_ref[pl.ds(sx * bx + R, bx)] += (METRIC[0][2] / METRIC[1][2]) * a
        a_ref[pl.ds(sx * bx, bx), pl.ds(Y0, ny), :] = a
        for i in range(bx):
            wrap_y(a_ref, sx * bx + i)
        wrap_x(c_ref, sx)

    many = 4 if bx % 4 == 0 and 4 % group == 0 else group
    tall = math.gcd(ny, 8)

    def x_rows(v, c_ref, x, y):
        vs = [v[x + i, pl.ds(Y0 + y, tall), :] for i in range(many + 2 * R)]
        cs = [c_ref[x + i, pl.ds(y, tall), :] for i in range(many + 2 * R)]
        totals = []
        for g in range(many):
            mid = g + R
            total = s_ref[x + g, pl.ds(y, tall), :] + p_ref[x + g, pl.ds(y, tall), :] * vs[mid]
            for k in range(1, R + 1):
                second = vs[mid + k] + vs[mid - k]
                first = (cs[mid + k] - cs[mid - k]) + (
                    a_ref[x + g, pl.ds(Y0 + y + k, tall), :]
                    - a_ref[x + g, pl.ds(Y0 + y - k, tall), :]
                )
                total = total + (-0.5 * METRIC[0][0] * SECOND[k]) * second
                total = total + FIRST[k - 1] * first
            totals.append(total)
        return totals

    def wait_all(copies):
        for copy in copies:
            copy.wait()

    block = [lax.rem(cx + gx + t - 2 * t * odd, gx) for t in range(gx)]

    def first_x_pass(t):
        sx = block[t]

        @pl.loop(0, bx // many)
        def _(i):
            x = sx * bx + i * many
            for y in range(0, ny, tall):
                for g, total in enumerate(x_rows(v0, c0, x, y)):
                    v1[x + g + R, pl.ds(Y0 + y, tall), :] = (1.0 / HALF_WIDTH) * total
            for g in range(many):
                wrap_y(v1, x + g + R)
        wrap_x(v1, sx)
        send_edges(1, v1, sx, t)
        y_pass(v1, c1, sx)

    far = list(range(gy // 2, gy))
    near = list(range(gy // 2))
    others = list(range(1, gx // 2))
    cross_order = far + near[::-1]

    own_pot.wait()
    soon = [send_pot(cy, (cx, across(d))) for d in masks]
    soon += [send_pot(cy, (x, cy)) for x in mates]
    send_band(partner, cy)
    send_group(0, [0], near + far)
    send_group(0, others, cross_order)
    z_matrix(bz, w_ref)
    for i in soon:
        wait_pot(i)
    later = [send_pot(across(d), (x, cy)) for x in mates for d in masks]
    reached = [0]
    hops = []
    for k, m in enumerate(masks):
        if k:
            hops.append((m, [o for o in reached if o]))
        reached = reached + [o ^ m for o in reached]

    def forward(hop):
        m, offsets = hop
        return [
            send_pot(across(o), (x, across(m))) for o in offsets for x in [cx] + mates
        ]

    hop = [i for h in hops[:1] for i in forward(h)]
    send_group(1, [0], near + far)
    send_group(1, others, cross_order)

    def enter(t):
        wait_block(block[t])
        assemble(block[t])
        send_edges(0, v0, block[t], t)
        y_pass(v0, c0, block[t])

    def enter_chip():
        for t in (0, 1):
            enter(t)
        for t in (0, 1):
            edge_wait(0, t)
            z_pass(0, v0, c0, block[t], t)

    pl.when(odd == 0)(enter_chip)
    for i in hop:
        wait_pot(i)
    for h in hops[1:]:
        for i in forward(h):
            wait_pot(i)
    for i in later:
        wait_pot(i)
    sharing = share_pot()
    pl.when(odd == 1)(enter_chip)
    for t in range(2, gx):
        enter(t)
    wait_all(sharing)
    assemble_potential()
    for t in range(2, gx - 1):
        edge_wait(0, t)
        z_pass(0, v0, c0, block[t], t)
    for t in range(1, gx - 2):
        first_x_pass(t)
    edge_wait(0, gx - 1)
    z_pass(0, v0, c0, block[gx - 1], gx - 1)
    for t in (gx - 2, gx - 1, 0):
        first_x_pass(t)

    own_out = []

    def last_x_pass(t):
        sx = block[t]

        @pl.loop(0, bx // many)
        def _(i):
            x = sx * bx + i * many
            at = pl.multiple_of(i * many * by, 8)
            for y in range(0, ny, tall):
                for g, total in enumerate(x_rows(v1, c1, x, y)):
                    got = (2.0 / HALF_WIDTH) * total - v0[x + g + R, pl.ds(Y0 + y, tall), :]
                    low = y
                    while low < y + tall:
                        sy = low // by
                        high = min(y + tall, (sy + 1) * by)
                        obuf[sx, sy, pl.ds(at + g * by + low - sy * by, high - low), :] = got[
                            low - y : high - y
                        ]
                        low = high

        for dy in cross_order:
            ty = across(dy)
            n = t * gy + dy
            if n == 0:
                own_out.append(
                    pltpu.make_async_copy(obuf.at[sx, ty], out.at[:, band], lsem.at[1])
                )
                own_out[0].start()
                continue
            copy = pltpu.make_async_remote_copy(
                obuf.at[sx, ty], out.at[:, band], osend.at[0], orecv.at[0],
                device_id=(sx, ty, cz), device_id_type=MESH,
            )
            copy.start()

    done = []
    for t in list(range(1, gx)) + [0]:
        edge_wait(1, t)
        z_pass(1, v1, c1, block[t], t)
        done.append(t)
        for u in range(gx):
            near = {u, (u + 1) % gx, (u - 1) % gx}
            if near <= set(done) and t in near:
                last_x_pass(u)
    own_out[0].wait()
    for copy in pot_out:
        copy.wait_send()
    meet(ebuf, hbuf, hsend.at[0], hrecv.at[0, 0]).wait_send()
    sent = vin.at[pl.ds(0, gx * gy - 1)]
    meet(sent, sent, isend.at[0], orecv.at[0]).wait_send()
    meet(sent, sent, osend.at[0], orecv.at[0]).wait_send()
    meet(sent, sent, osend.at[0], orecv.at[0]).wait_recv()


def local(sizes, orbitals, potential):
    gx, gy, gz = sizes
    bands, bx, by, bz = orbitals.shape
    nx, ny = gx * bx, gy * by
    assert bands == gx * gy and gz > 1 and gx >= 4 and gx & (gx - 1) == 0
    assert gy >= 2 and gy & (gy - 1) == 0
    f32 = jnp.float32
    anywhere = pl.BlockSpec(memory_space=pl.ANY)
    dma = pltpu.SemaphoreType.DMA
    hops, mates = gy.bit_length() - 1, gx // 2 - 1
    pots = hops + mates + hops * mates + (1 + mates) * sum(2**k - 1 for k in range(1, hops))
    edge = (DEGREE, gx, 2, 8, (bx * ny + 127) // 128 * 128)
    out = pl.pallas_call(
        functools.partial(kernel, gx, gy, gz, bx, by),
        out_shape=jax.ShapeDtypeStruct((bx * by, bands, bz), f32),
        in_specs=[anywhere] * 2,
        out_specs=anywhere,
        scratch_shapes=[
            pltpu.VMEM((3 * bz + 128, 2 * bz), jnp.bfloat16),
            pltpu.VMEM((gx * gy, bx * by, bz), f32),
            pltpu.VMEM((gx, gy, bx, by, bz), f32),
            pltpu.VMEM((nx, ny, bz), f32),
            pltpu.VMEM((nx + 2 * R, ny + 16, bz), f32),
            pltpu.VMEM((nx + 2 * R, ny + 16, bz), f32),
            pltpu.VMEM((nx, ny + 16, bz), f32),
            pltpu.VMEM((nx + 2 * R, ny, bz), f32),
            pltpu.VMEM((nx + 2 * R, ny, bz), f32),
            pltpu.VMEM((nx, ny, bz), f32),
            pltpu.VMEM((gx, gy, bx * by, bz), f32),
            pltpu.VMEM(edge, f32),
            pltpu.VMEM(edge, f32),
            dma((1,)), dma((gx,)),
            dma((pots,)), dma((pots,)),
            dma((gx // 2,)), dma((gx // 2,)),
            dma((1,)), dma((DEGREE, gx)),
            dma((1,)), dma((1,)),
            dma((2,)),
        ],
        compiler_params=pltpu.CompilerParams(
            collective_id=0, has_side_effects=True, vmem_limit_bytes=48 * 1024 * 1024
        ),
    )(
        pltpu.with_memory_space_constraint(
            orbitals.transpose(1, 2, 0, 3).reshape(bx * by, bands, bz), pltpu.HBM
        ),
        pltpu.with_memory_space_constraint(potential, pltpu.HBM),
    )
    return out.reshape(bx, by, bands, bz).transpose(2, 0, 1, 3)


def solution(mesh):
    sizes = tuple(mesh.shape[a] for a in ("gx", "gy", "gz"))
    return jax.shard_map(
        functools.partial(local, sizes),
        mesh=mesh,
        in_specs=(P(None, "gx", "gy", "gz"), P("gx", "gy", "gz")),
        out_specs=P(None, "gx", "gy", "gz"),
        check_vma=False,
    )
```

```python
import functools
import math

import jax
import jax.numpy as jnp
import numpy as np
from jax import lax
from jax.experimental import pallas as pl
from jax.experimental.pallas import tpu as pltpu
from jax.sharding import PartitionSpec as P

DEGREE = 2
SECOND = (
    -5369.0 / 1800.0,
    12.0 / 7.0,
    -15.0 / 56.0,
    10.0 / 189.0,
    -1.0 / 112.0,
    2.0 / 1925.0,
    -1.0 / 16632.0,
)
FIRST = (6.0 / 7.0, -15.0 / 56.0, 5.0 / 63.0, -1.0 / 56.0, 3.0 / 385.0, -1.0 / 792.0)
METRIC = ((1.0, 0.25, 0.15), (0.25, 1.0, 0.2), (0.15, 0.2, 1.0))
CENTER = 10.5
HALF_WIDTH = 9.5
R = 6
Y0 = 8
MESH = pl.DeviceIdType.MESH


def halves(x):
    high = float(np.float32(x).astype(jnp.bfloat16))
    return high, float(np.float32(x - high).astype(jnp.bfloat16))


def bands_of(offset, part):
    out = []
    cross = [-METRIC[1][2] * c for c in FIRST]
    for table, sign in ((cross, -1.0), ([-0.5 * METRIC[2][2] * c for c in SECOND[1:]], 1.0)):
        acc = jnp.zeros(offset.shape, jnp.float32)
        for k in range(1, R + 1):
            value = halves(table[k - 1])[part]
            acc = jnp.where(offset == k, value, acc)
            acc = jnp.where(offset == -k, sign * value, acc)
        out.append(acc)
    return jnp.concatenate(out, axis=1).astype(jnp.bfloat16)


def z_matrix(bz, w_ref):
    def index(shape, dim):
        return lax.broadcasted_iota(jnp.int32, shape, dim)

    square, edge = (bz, bz), (16, bz)
    offset = index(square, 0) - index(square, 1)
    e = index(edge, 0)
    beyond = jnp.where(e < 8, e - 8, e - 8 + bz) - index(edge, 1)
    high, edge_high = bands_of(offset, 0), bands_of(beyond, 0)
    parts = [high, high, bands_of(offset, 1), edge_high, edge_high, bands_of(beyond, 1)]
    parts.append(jnp.zeros((80, 2 * bz), jnp.bfloat16))
    at = 0
    for part in parts:
        w_ref[pl.ds(at, part.shape[0]), :] = part
        at += part.shape[0]


def kernel(
    gx, gy, gz, bx, by,
    orb, pot, out,
    w_ref, vin, pin, p_ref, v0, v1, a_ref, c0, c1, s_ref, obuf, ebuf, hbuf,
    isend, irecv, psend, precv, qsend, qrecv, hsend, hrecv, osend, orecv, lsem,
):
    bz = orb.shape[-1]
    nx, ny = gx * bx, gy * by
    group = 8 // math.gcd(by, 8)
    rows = bx * ny
    padded_rows = ebuf.shape[-1]
    tall = math.gcd(ny, 8)
    cx, cy, cz = lax.axis_index("gx"), lax.axis_index("gy"), lax.axis_index("gz")
    band = cx * gy + cy
    zl, zr = lax.rem(cz + gz - 1, gz), lax.rem(cz + 1, gz)
    odd = lax.rem(cx, 2)
    chip = cx - odd
    partner = chip + 1 - odd

    def across(d):
        ty, bit = cy, 1
        while bit <= d:
            if d & bit:
                ty = ty + bit - 2 * bit * lax.rem(lax.div(cy, bit), 2)
            bit *= 2
        return ty

    far_first = list(range(gy - 1, 0, -1))

    own_pot = pltpu.make_async_copy(pot, pin.at[cx, cy], lsem.at[0])
    own_pot.start()
    own_band = pltpu.make_async_copy(orb.at[:, band], vin.at[band], irecv.at[cx])
    own_band.start()
    for step in range(DEGREE):
        for t in range(gx):
            hbuf[step, t, 0, pl.ds(0, 8 - R), :] = jnp.zeros((8 - R, padded_rows), jnp.float32)
            hbuf[step, t, 1, pl.ds(R, 8 - R), :] = jnp.zeros((8 - R, padded_rows), jnp.float32)
    barrier = pltpu.get_barrier_semaphore()
    for dx in range(gx):
        for dy in range(gy):
            if dx or dy:
                pl.semaphore_signal(
                    barrier, inc=1,
                    device_id=(lax.rem(cx + dx, gx), lax.rem(cy + dy, gy), cz),
                    device_id_type=MESH,
                )
    for z in (zl, zr):
        pl.semaphore_signal(barrier, inc=1, device_id=(cx, cy, z), device_id_type=MESH)
    pl.semaphore_wait(barrier, gx * gy + 1)

    masks = []
    m = gy - 1
    while m:
        masks.append(m)
        m //= 2
    mates = [lax.rem(cx + 2 * i, gx) for i in range(1, gx // 2)]
    pot_out = []

    def send_pot(y, target):
        i = len(pot_out)
        copy = pltpu.make_async_remote_copy(
            pin.at[cx, y], pin.at[cx, y], psend.at[i], precv.at[i],
            device_id=target + (cz,), device_id_type=MESH,
        )
        copy.start()
        pot_out.append(copy)
        return i

    def wait_pot(i):
        pot_out[i].wait_recv()

    def share_pot():
        copies = []
        for i, x in enumerate([cx] + mates):
            copy = pltpu.make_async_remote_copy(
                pin.at[x], pin.at[x], qsend.at[i], qrecv.at[i],
                device_id=(partner, cy, cz), device_id_type=MESH,
            )
            copy.start()
            copies.append(copy)
        return copies

    def meet(src, dst, send, recv):
        return pltpu.make_async_remote_copy(
            src, dst, send, recv, device_id=(partner, cy, cz), device_id_type=MESH
        )

    def send_band(tx, ty):
        pltpu.make_async_remote_copy(
            orb.at[:, tx * gy + ty], vin.at[band], isend.at[0], irecv.at[cx],
            device_id=(tx, ty, cz), device_id_type=MESH,
        ).start()

    def send_group(g, pairs, ds):
        for d in ds:
            for i in pairs:
                if i or d:
                    send_band(lax.rem(chip + 2 * i + g, gx), across(d))

    def wait_block(sx):
        blocks = vin.at[pl.ds(sx * gy, gy)]
        meet(blocks, blocks, isend.at[0], irecv.at[sx]).wait_recv()

    def wrap_y(ref, x):
        ref[x, pl.ds(Y0 - R, R), :] = ref[x, pl.ds(Y0 + ny - R, R), :]
        ref[x, pl.ds(Y0 + ny, R), :] = ref[x, pl.ds(Y0, R), :]

    def wrap_x(ref, sx):
        @pl.when(sx == 0)
        def _():
            ref[pl.ds(nx + R, R)] = ref[pl.ds(R, R)]

        @pl.when(sx == gx - 1)
        def _():
            ref[pl.ds(0, R)] = ref[pl.ds(nx, R)]

    def pieces(sx, i):
        at = pl.multiple_of(i * group * by, 8)
        for sy in range(gy):
            got = vin[sx * gy + sy, pl.ds(at, group * by), :]
            for j in range(group):
                yield sy, j, got[j * by : (j + 1) * by]

    def assemble(sx):
        @pl.loop(0, bx // group)
        def _(i):
            x = sx * bx + i * group + R
            for sy, j, piece in pieces(sx, i):
                v0[x + j, pl.ds(Y0 + sy * by, by), :] = piece
            for j in range(group):
                wrap_y(v0, x + j)
        wrap_x(v0, sx)

    def assemble_potential():
        for sx in range(gx):
            @pl.loop(0, bx)
            def _(i):
                for sy in range(gy):
                    p_ref[sx * bx + i, pl.ds(sy * by, by), :] = pin[sx, sy, i] + (
                        -1.5 * SECOND[0] - CENTER
                    )

    def edge_wait(step, t):
        edges = hbuf.at[step, t, :, pl.ds(0, R)]
        meet(edges, edges, hsend.at[0], hrecv.at[step, t]).wait_recv()

    def edge_copies(step, t):
        return [
            pltpu.make_async_remote_copy(
                ebuf.at[step, t, side, pl.ds(2 * side, R)],
                hbuf.at[step, t, 1 - side, pl.ds(2 * side, R)],
                hsend.at[0], hrecv.at[step, t],
                device_id=(cx, cy, z), device_id_type=MESH,
            )
            for side, z in ((0, zl), (1, zr))
        ]

    def send_edges(step, v, sx, t):
        vals = v[pl.ds(sx * bx + R, bx), pl.ds(Y0, ny), :].reshape(rows, bz)
        if padded_rows > rows:
            vals = jnp.concatenate([vals, jnp.zeros((padded_rows - rows, bz), jnp.float32)], axis=0)
        for i in range(padded_rows // 128):
            turned = vals[i * 128 : (i + 1) * 128].T
            ebuf[step, t, 0, :, pl.ds(i * 128, 128)] = turned[:8]
            ebuf[step, t, 1, :, pl.ds(i * 128, 128)] = turned[bz - 8 :]
        for copy in edge_copies(step, t):
            copy.start()

    def y_pass(v, c_ref, sx):
        @pl.loop(0, bx // group)
        def _(i):
            for j in range(group):
                x = sx * bx + i * group + j
                for y in range(0, ny, tall):
                    first = second = None
                    for k in range(1, R + 1):
                        up = v[x + R, pl.ds(Y0 + y + k, tall), :]
                        down = v[x + R, pl.ds(Y0 + y - k, tall), :]
                        f = (-METRIC[0][1] * FIRST[k - 1]) * (up - down)
                        s = (-0.5 * METRIC[1][1] * SECOND[k]) * (up + down)
                        first = f if first is None else first + f
                        second = s if second is None else second + s
                    c_ref[x + R, pl.ds(y, tall), :] = first
                    s_ref[x, pl.ds(y, tall), :] = second

    def split(x):
        high = x.astype(jnp.bfloat16)
        return high, (x - high.astype(jnp.float32)).astype(jnp.bfloat16)

    def z_pass(step, v, c_ref, sx, t):
        vals = v[pl.ds(sx * bx + R, bx), pl.ds(Y0, ny), :].reshape(rows, bz)
        high, low = split(vals)
        sides = []
        for i in range(padded_rows // 128):
            edge = jnp.concatenate(
                [hbuf[step, t, side, :, pl.ds(i * 128, 128)] for side in (0, 1)], axis=0
            )
            eh, el = (e.astype(jnp.float32) for e in split(edge))
            block = jnp.concatenate([eh, el, eh, jnp.zeros((80, 128), jnp.float32)], axis=0)
            sides.append(block.T.astype(jnp.bfloat16))
        side = jnp.concatenate(sides, axis=0)[:rows]
        got = jnp.dot(
            jnp.concatenate([high, low, high, side], axis=1), w_ref[...],
            preferred_element_type=jnp.float32,
        )
        a = got[:, :bz].reshape(bx, ny, bz)
        s_ref[pl.ds(sx * bx, bx)] += got[:, bz:].reshape(bx, ny, bz)
        c_ref[pl.ds(sx * bx + R, bx)] += (METRIC[0][2] / METRIC[1][2]) * a
        a_ref[pl.ds(sx * bx, bx), pl.ds(Y0, ny), :] = a
        for i in range(bx):
            wrap_y(a_ref, sx * bx + i)
        wrap_x(c_ref, sx)

    many = 4 if bx % 4 == 0 and 4 % group == 0 else group

    def along_x(v, x, y):
        vs = [v[x + i, pl.ds(Y0 + y, tall), :] for i in range(many + 2 * R)]
        totals = []
        for g in range(many):
            mid = g + R
            total = s_ref[x + g, pl.ds(y, tall), :] + p_ref[x + g, pl.ds(y, tall), :] * vs[mid]
            for k in range(1, R + 1):
                second = vs[mid + k] + vs[mid - k]
                total = total + (-0.5 * METRIC[0][0] * SECOND[k]) * second
            totals.append(total)
        return totals

    def crossed(c_ref, x, y, totals):
        cs = [c_ref[x + i, pl.ds(y, tall), :] for i in range(many + 2 * R)]
        out = []
        for g, total in enumerate(totals):
            mid = g + R
            for k in range(1, R + 1):
                first = (cs[mid + k] - cs[mid - k]) + (
                    a_ref[x + g, pl.ds(Y0 + y + k, tall), :]
                    - a_ref[x + g, pl.ds(Y0 + y - k, tall), :]
                )
                total = total + FIRST[k - 1] * first
            out.append(total)
        return out

    def before_edges(sx):
        @pl.loop(0, bx // many)
        def _(i):
            x = sx * bx + i * many
            for y in range(0, ny, tall):
                for g, total in enumerate(along_x(v0, x, y)):
                    s_ref[x + g, pl.ds(y, tall), :] = total

    def wait_all(copies):
        for copy in copies:
            copy.wait()

    block = [lax.rem(cx + gx + t - 2 * t * odd, gx) for t in range(gx)]

    def first_x_pass(t):
        sx = block[t]

        @pl.loop(0, bx // many)
        def _(i):
            x = sx * bx + i * many
            for y in range(0, ny, tall):
                totals = [s_ref[x + g, pl.ds(y, tall), :] for g in range(many)]
                for g, total in enumerate(crossed(c0, x, y, totals)):
                    v1[x + g + R, pl.ds(Y0 + y, tall), :] = (1.0 / HALF_WIDTH) * total
            for g in range(many):
                wrap_y(v1, x + g + R)
        wrap_x(v1, sx)
        send_edges(1, v1, sx, t)
        y_pass(v1, c1, sx)

    far = list(range(gy // 2, gy))
    near = list(range(gy // 2))
    others = list(range(1, gx // 2))
    cross_order = far + near[::-1]

    own_pot.wait()
    soon = [send_pot(cy, (cx, across(d))) for d in masks]
    soon += [send_pot(cy, (x, cy)) for x in mates]
    send_band(partner, cy)
    send_group(0, [0], near + far)
    send_group(0, others, cross_order)
    z_matrix(bz, w_ref)
    for i in soon:
        wait_pot(i)
    later = [send_pot(across(d), (x, cy)) for x in mates for d in masks]
    reached = [0]
    hops = []
    for k, m in enumerate(masks):
        if k:
            hops.append((m, [o for o in reached if o]))
        reached = reached + [o ^ m for o in reached]

    def forward(hop):
        m, offsets = hop
        return [
            send_pot(across(o), (x, across(m))) for o in offsets for x in [cx] + mates
        ]

    hop = [i for h in hops[:1] for i in forward(h)]
    send_group(1, [0], near + far)
    send_group(1, others, cross_order)

    def enter(t):
        wait_block(block[t])
        assemble(block[t])
        send_edges(0, v0, block[t], t)
        y_pass(v0, c0, block[t])

    def enter_chip():
        for t in (0, 1):
            enter(t)
        for t in (0, 1):
            edge_wait(0, t)
            z_pass(0, v0, c0, block[t], t)

    pl.when(odd == 0)(enter_chip)
    for i in hop:
        wait_pot(i)
    for h in hops[1:]:
        for i in forward(h):
            wait_pot(i)
    for i in later:
        wait_pot(i)
    sharing = share_pot()
    pl.when(odd == 1)(enter_chip)
    for t in range(2, gx):
        enter(t)
    wait_all(sharing)
    assemble_potential()
    for t in range(gx):
        before_edges(block[t])
    for t in range(2, gx - 1):
        edge_wait(0, t)
        z_pass(0, v0, c0, block[t], t)
    for t in range(1, gx - 2):
        first_x_pass(t)
    edge_wait(0, gx - 1)
    z_pass(0, v0, c0, block[gx - 1], gx - 1)
    for t in (gx - 2, gx - 1, 0):
        first_x_pass(t)

    own_out = []

    def last_x_pass(t):
        sx = block[t]

        @pl.loop(0, bx // many)
        def _(i):
            x = sx * bx + i * many
            at = pl.multiple_of(i * many * by, 8)
            for y in range(0, ny, tall):
                for g, total in enumerate(crossed(c1, x, y, along_x(v1, x, y))):
                    got = (2.0 / HALF_WIDTH) * total - v0[x + g + R, pl.ds(Y0 + y, tall), :]
                    low = y
                    while low < y + tall:
                        sy = low // by
                        high = min(y + tall, (sy + 1) * by)
                        obuf[sx, sy, pl.ds(at + g * by + low - sy * by, high - low), :] = got[
                            low - y : high - y
                        ]
                        low = high

        for dy in cross_order:
            ty = across(dy)
            n = t * gy + dy
            if n == 0:
                own_out.append(
                    pltpu.make_async_copy(obuf.at[sx, ty], out.at[:, band], lsem.at[1])
                )
                own_out[0].start()
                continue
            copy = pltpu.make_async_remote_copy(
                obuf.at[sx, ty], out.at[:, band], osend.at[0], orecv.at[0],
                device_id=(sx, ty, cz), device_id_type=MESH,
            )
            copy.start()

    done = []
    for t in list(range(1, gx)) + [0]:
        edge_wait(1, t)
        z_pass(1, v1, c1, block[t], t)
        done.append(t)
        for u in range(gx):
            near = {u, (u + 1) % gx, (u - 1) % gx}
            if near <= set(done) and t in near:
                last_x_pass(u)
    own_out[0].wait()
    for copy in pot_out:
        copy.wait_send()
    edges = ebuf.at[:, :, :, pl.ds(0, R)]
    meet(edges, edges, hsend.at[0], hrecv.at[0, 0]).wait_send()
    sent = vin.at[pl.ds(0, gx * gy - 1)]
    meet(sent, sent, isend.at[0], orecv.at[0]).wait_send()
    meet(sent, sent, osend.at[0], orecv.at[0]).wait_send()
    meet(sent, sent, osend.at[0], orecv.at[0]).wait_recv()


def local(sizes, orbitals, potential):
    gx, gy, gz = sizes
    bands, bx, by, bz = orbitals.shape
    nx, ny = gx * bx, gy * by
    assert bands == gx * gy and gz > 1 and gx >= 4 and gx & (gx - 1) == 0
    assert gy >= 2 and gy & (gy - 1) == 0
    f32 = jnp.float32
    anywhere = pl.BlockSpec(memory_space=pl.ANY)
    dma = pltpu.SemaphoreType.DMA
    hops, mates = gy.bit_length() - 1, gx // 2 - 1
    pots = hops + mates + hops * mates + (1 + mates) * sum(2**k - 1 for k in range(1, hops))
    edge = (DEGREE, gx, 2, 8, (bx * ny + 127) // 128 * 128)
    out = pl.pallas_call(
        functools.partial(kernel, gx, gy, gz, bx, by),
        out_shape=jax.ShapeDtypeStruct((bx * by, bands, bz), f32),
        in_specs=[anywhere] * 2,
        out_specs=anywhere,
        scratch_shapes=[
            pltpu.VMEM((3 * bz + 128, 2 * bz), jnp.bfloat16),
            pltpu.VMEM((gx * gy, bx * by, bz), f32),
            pltpu.VMEM((gx, gy, bx, by, bz), f32),
            pltpu.VMEM((nx, ny, bz), f32),
            pltpu.VMEM((nx + 2 * R, ny + 16, bz), f32),
            pltpu.VMEM((nx + 2 * R, ny + 16, bz), f32),
            pltpu.VMEM((nx, ny + 16, bz), f32),
            pltpu.VMEM((nx + 2 * R, ny, bz), f32),
            pltpu.VMEM((nx + 2 * R, ny, bz), f32),
            pltpu.VMEM((nx, ny, bz), f32),
            pltpu.VMEM((gx, gy, bx * by, bz), f32),
            pltpu.VMEM(edge, f32),
            pltpu.VMEM(edge, f32),
            dma((1,)), dma((gx,)),
            dma((pots,)), dma((pots,)),
            dma((gx // 2,)), dma((gx // 2,)),
            dma((1,)), dma((DEGREE, gx)),
            dma((1,)), dma((1,)),
            dma((2,)),
        ],
        compiler_params=pltpu.CompilerParams(
            collective_id=0, has_side_effects=True, vmem_limit_bytes=48 * 1024 * 1024
        ),
    )(
        pltpu.with_memory_space_constraint(
            orbitals.transpose(1, 2, 0, 3).reshape(bx * by, bands, bz), pltpu.HBM
        ),
        pltpu.with_memory_space_constraint(potential, pltpu.HBM),
    )
    return out.reshape(bx, by, bands, bz).transpose(2, 0, 1, 3)


def solution(mesh):
    sizes = tuple(mesh.shape[a] for a in ("gx", "gy", "gz"))
    return jax.shard_map(
        functools.partial(local, sizes),
        mesh=mesh,
        in_specs=(P(None, "gx", "gy", "gz"), P("gx", "gy", "gz")),
        out_specs=P(None, "gx", "gy", "gz"),
        check_vma=False,
    )
```

```python
import functools
import math

import jax
import jax.numpy as jnp
import numpy as np
from jax import lax
from jax.experimental import pallas as pl
from jax.experimental.pallas import tpu as pltpu
from jax.sharding import PartitionSpec as P

DEGREE = 2
SECOND = (
    -5369.0 / 1800.0,
    12.0 / 7.0,
    -15.0 / 56.0,
    10.0 / 189.0,
    -1.0 / 112.0,
    2.0 / 1925.0,
    -1.0 / 16632.0,
)
FIRST = (6.0 / 7.0, -15.0 / 56.0, 5.0 / 63.0, -1.0 / 56.0, 3.0 / 385.0, -1.0 / 792.0)
METRIC = ((1.0, 0.25, 0.15), (0.25, 1.0, 0.2), (0.15, 0.2, 1.0))
CENTER = 10.5
HALF_WIDTH = 9.5
R = 6
Y0 = 8
MESH = pl.DeviceIdType.MESH


def halves(x):
    high = float(np.float32(x).astype(jnp.bfloat16))
    return high, float(np.float32(x - high).astype(jnp.bfloat16))


def bands_of(offset, part):
    out = []
    cross = [-METRIC[1][2] * c for c in FIRST]
    for table, sign in ((cross, -1.0), ([-0.5 * METRIC[2][2] * c for c in SECOND[1:]], 1.0)):
        acc = jnp.zeros(offset.shape, jnp.float32)
        for k in range(1, R + 1):
            value = halves(table[k - 1])[part]
            acc = jnp.where(offset == k, value, acc)
            acc = jnp.where(offset == -k, sign * value, acc)
        out.append(acc)
    return jnp.concatenate(out, axis=1).astype(jnp.bfloat16)


def z_matrix(bz, w_ref):
    def index(shape, dim):
        return lax.broadcasted_iota(jnp.int32, shape, dim)

    square, edge = (bz, bz), (16, bz)
    offset = index(square, 0) - index(square, 1)
    e = index(edge, 0)
    beyond = jnp.where(e < 8, e - 8, e - 8 + bz) - index(edge, 1)
    high, edge_high = bands_of(offset, 0), bands_of(beyond, 0)
    parts = [high, high, bands_of(offset, 1), edge_high, edge_high, bands_of(beyond, 1)]
    parts.append(jnp.zeros((80, 2 * bz), jnp.bfloat16))
    at = 0
    for part in parts:
        w_ref[pl.ds(at, part.shape[0]), :] = part
        at += part.shape[0]


def kernel(
    gx, gy, gz, bx, by,
    orb, pot, out,
    w_ref, vin, pin, p_ref, v0, v1, a_ref, c0, c1, s_ref, obuf, ebuf, hbuf,
    isend, irecv, psend, precv, qsend, qrecv, hsend, hrecv, osend, orecv, lsem,
):
    bz = orb.shape[-1]
    nx, ny = gx * bx, gy * by
    group = 8 // math.gcd(by, 8)
    rows = bx * ny
    padded_rows = ebuf.shape[-1]
    tall = math.gcd(ny, 8)
    cx, cy, cz = lax.axis_index("gx"), lax.axis_index("gy"), lax.axis_index("gz")
    band = cx * gy + cy
    zl, zr = lax.rem(cz + gz - 1, gz), lax.rem(cz + 1, gz)
    odd = lax.rem(cx, 2)
    chip = cx - odd
    partner = chip + 1 - odd

    def across(d):
        ty, bit = cy, 1
        while bit <= d:
            if d & bit:
                ty = ty + bit - 2 * bit * lax.rem(lax.div(cy, bit), 2)
            bit *= 2
        return ty

    far_first = list(range(gy - 1, 0, -1))

    own_pot = pltpu.make_async_copy(pot, pin.at[cx, cy], lsem.at[0])
    own_pot.start()
    own_band = pltpu.make_async_copy(orb.at[:, band], vin.at[band], irecv.at[cx])
    own_band.start()
    for step in range(DEGREE):
        for t in range(gx):
            hbuf[step, t, 0, pl.ds(0, 8 - R), :] = jnp.zeros((8 - R, padded_rows), jnp.float32)
            hbuf[step, t, 1, pl.ds(R, 8 - R), :] = jnp.zeros((8 - R, padded_rows), jnp.float32)
    barrier = pltpu.get_barrier_semaphore()
    for dx in range(gx):
        for dy in range(gy):
            if dx or dy:
                pl.semaphore_signal(
                    barrier, inc=1,
                    device_id=(lax.rem(cx + dx, gx), lax.rem(cy + dy, gy), cz),
                    device_id_type=MESH,
                )
    for z in (zl, zr):
        pl.semaphore_signal(barrier, inc=1, device_id=(cx, cy, z), device_id_type=MESH)
    pl.semaphore_wait(barrier, gx * gy + 1)

    masks = []
    m = gy - 1
    while m:
        masks.append(m)
        m //= 2
    mates = [lax.rem(cx + 2 * i, gx) for i in range(1, gx // 2)]
    pot_out = []

    def send_pot(y, target):
        i = len(pot_out)
        copy = pltpu.make_async_remote_copy(
            pin.at[cx, y], pin.at[cx, y], psend.at[i], precv.at[i],
            device_id=target + (cz,), device_id_type=MESH,
        )
        copy.start()
        pot_out.append(copy)
        return i

    def wait_pot(i):
        pot_out[i].wait_recv()

    def share_pot():
        copies = []
        for i, x in enumerate([cx] + mates):
            copy = pltpu.make_async_remote_copy(
                pin.at[x], pin.at[x], qsend.at[i], qrecv.at[i],
                device_id=(partner, cy, cz), device_id_type=MESH,
            )
            copy.start()
            copies.append(copy)
        return copies

    def meet(src, dst, send, recv):
        return pltpu.make_async_remote_copy(
            src, dst, send, recv, device_id=(partner, cy, cz), device_id_type=MESH
        )

    def send_band(tx, ty):
        pltpu.make_async_remote_copy(
            orb.at[:, tx * gy + ty], vin.at[band], isend.at[0], irecv.at[cx],
            device_id=(tx, ty, cz), device_id_type=MESH,
        ).start()

    def send_group(g, pairs, ds):
        for d in ds:
            for i in pairs:
                if i or d:
                    send_band(lax.rem(chip + 2 * i + g, gx), across(d))

    def wait_block(sx):
        blocks = vin.at[pl.ds(sx * gy, gy)]
        meet(blocks, blocks, isend.at[0], irecv.at[sx]).wait_recv()

    def wrap_y(ref, x):
        ref[x, pl.ds(Y0 - R, R), :] = ref[x, pl.ds(Y0 + ny - R, R), :]
        ref[x, pl.ds(Y0 + ny, R), :] = ref[x, pl.ds(Y0, R), :]

    def wrap_x(ref, sx):
        @pl.when(sx == 0)
        def _():
            ref[pl.ds(nx + R, R)] = ref[pl.ds(R, R)]

        @pl.when(sx == gx - 1)
        def _():
            ref[pl.ds(0, R)] = ref[pl.ds(nx, R)]

    def pieces(sx, i):
        at = pl.multiple_of(i * group * by, 8)
        for sy in range(gy):
            got = vin[sx * gy + sy, pl.ds(at, group * by), :]
            for j in range(group):
                yield sy, j, got[j * by : (j + 1) * by]

    def assemble(sx):
        @pl.loop(0, bx // group)
        def _(i):
            x = sx * bx + i * group + R
            for sy, j, piece in pieces(sx, i):
                v0[x + j, pl.ds(Y0 + sy * by, by), :] = piece
            for j in range(group):
                wrap_y(v0, x + j)
        wrap_x(v0, sx)

    def assemble_potential():
        for sx in range(gx):
            @pl.loop(0, bx)
            def _(i):
                for sy in range(gy):
                    p_ref[sx * bx + i, pl.ds(sy * by, by), :] = pin[sx, sy, i] + (
                        -1.5 * SECOND[0] - CENTER
                    )

    def edge_wait(step, t):
        edges = hbuf.at[step, t, :, pl.ds(0, R)]
        meet(edges, edges, hsend.at[0], hrecv.at[step, t]).wait_recv()

    def edge_copies(step, t):
        return [
            pltpu.make_async_remote_copy(
                ebuf.at[step, t, side, pl.ds(2 * side, R)],
                hbuf.at[step, t, 1 - side, pl.ds(2 * side, R)],
                hsend.at[0], hrecv.at[step, t],
                device_id=(cx, cy, z), device_id_type=MESH,
            )
            for side, z in ((0, zl), (1, zr))
        ]

    def send_edges(step, v, sx, t):
        vals = v[pl.ds(sx * bx + R, bx), pl.ds(Y0, ny), :].reshape(rows, bz)
        if padded_rows > rows:
            vals = jnp.concatenate([vals, jnp.zeros((padded_rows - rows, bz), jnp.float32)], axis=0)
        for i in range(padded_rows // 128):
            turned = vals[i * 128 : (i + 1) * 128].T
            ebuf[step, t, 0, :, pl.ds(i * 128, 128)] = turned[:8]
            ebuf[step, t, 1, :, pl.ds(i * 128, 128)] = turned[bz - 8 :]
        for copy in edge_copies(step, t):
            copy.start()

    def y_pass(v, c_ref, sx):
        @pl.loop(0, bx // group)
        def _(i):
            for j in range(group):
                x = sx * bx + i * group + j
                for y in range(0, ny, tall):
                    first = second = None
                    for k in range(1, R + 1):
                        up = v[x + R, pl.ds(Y0 + y + k, tall), :]
                        down = v[x + R, pl.ds(Y0 + y - k, tall), :]
                        f = (-METRIC[0][1] * FIRST[k - 1]) * (up - down)
                        s = (-0.5 * METRIC[1][1] * SECOND[k]) * (up + down)
                        first = f if first is None else first + f
                        second = s if second is None else second + s
                    c_ref[x + R, pl.ds(y, tall), :] = first
                    s_ref[x, pl.ds(y, tall), :] = second

    def split(x):
        high = x.astype(jnp.bfloat16)
        return high, (x - high.astype(jnp.float32)).astype(jnp.bfloat16)

    def z_pass(step, v, c_ref, sx, t):
        vals = v[pl.ds(sx * bx + R, bx), pl.ds(Y0, ny), :].reshape(rows, bz)
        high, low = split(vals)
        sides = []
        for i in range(padded_rows // 128):
            edge = jnp.concatenate(
                [hbuf[step, t, side, :, pl.ds(i * 128, 128)] for side in (0, 1)], axis=0
            )
            eh, el = (e.astype(jnp.float32) for e in split(edge))
            block = jnp.concatenate([eh, el, eh, jnp.zeros((80, 128), jnp.float32)], axis=0)
            sides.append(block.T.astype(jnp.bfloat16))
        side = jnp.concatenate(sides, axis=0)[:rows]
        got = jnp.dot(
            jnp.concatenate([high, low, high, side], axis=1), w_ref[...],
            preferred_element_type=jnp.float32,
        )
        a = got[:, :bz].reshape(bx, ny, bz)
        s_ref[pl.ds(sx * bx, bx)] += got[:, bz:].reshape(bx, ny, bz)
        c_ref[pl.ds(sx * bx + R, bx)] += (METRIC[0][2] / METRIC[1][2]) * a
        a_ref[pl.ds(sx * bx, bx), pl.ds(Y0, ny), :] = a
        for i in range(bx):
            wrap_y(a_ref, sx * bx + i)
        wrap_x(c_ref, sx)

    many = 4 if bx % 4 == 0 and 4 % group == 0 else group

    def along_x(v, x, y):
        vs = [v[x + i, pl.ds(Y0 + y, tall), :] for i in range(many + 2 * R)]
        totals = []
        for g in range(many):
            mid = g + R
            total = s_ref[x + g, pl.ds(y, tall), :] + p_ref[x + g, pl.ds(y, tall), :] * vs[mid]
            for k in range(1, R + 1):
                second = vs[mid + k] + vs[mid - k]
                total = total + (-0.5 * METRIC[0][0] * SECOND[k]) * second
            totals.append(total)
        return totals

    def crossed(c_ref, x, y, totals):
        cs = [c_ref[x + i, pl.ds(y, tall), :] for i in range(many + 2 * R)]
        out = []
        for g, total in enumerate(totals):
            mid = g + R
            for k in range(1, R + 1):
                first = (cs[mid + k] - cs[mid - k]) + (
                    a_ref[x + g, pl.ds(Y0 + y + k, tall), :]
                    - a_ref[x + g, pl.ds(Y0 + y - k, tall), :]
                )
                total = total + FIRST[k - 1] * first
            out.append(total)
        return out

    def before_edges(sx):
        @pl.loop(0, bx // many)
        def _(i):
            x = sx * bx + i * many
            for y in range(0, ny, tall):
                for g, total in enumerate(along_x(v0, x, y)):
                    s_ref[x + g, pl.ds(y, tall), :] = total

    def wait_all(copies):
        for copy in copies:
            copy.wait()

    block = [lax.rem(cx + gx + t - 2 * t * odd, gx) for t in range(gx)]

    def first_x_pass(t):
        sx = block[t]

        @pl.loop(0, bx // many)
        def _(i):
            x = sx * bx + i * many
            for y in range(0, ny, tall):
                totals = [s_ref[x + g, pl.ds(y, tall), :] for g in range(many)]
                for g, total in enumerate(crossed(c0, x, y, totals)):
                    v1[x + g + R, pl.ds(Y0 + y, tall), :] = (1.0 / HALF_WIDTH) * total
            for g in range(many):
                wrap_y(v1, x + g + R)
        wrap_x(v1, sx)
        send_edges(1, v1, sx, t)
        y_pass(v1, c1, sx)

    far = list(range(gy // 2, gy))
    near = list(range(gy // 2))
    others = list(range(1, gx // 2))
    cross_order = far + near[::-1]

    own_pot.wait()
    soon = [send_pot(cy, (cx, across(d))) for d in masks]
    soon += [send_pot(cy, (x, cy)) for x in mates]
    send_band(partner, cy)
    send_group(1, [0], near + far)
    send_group(1, others, near + far)
    z_matrix(bz, w_ref)
    for i in soon:
        wait_pot(i)
    later = [send_pot(across(d), (x, cy)) for x in mates for d in masks]
    reached = [0]
    hops = []
    for k, m in enumerate(masks):
        if k:
            hops.append((m, [o for o in reached if o]))
        reached = reached + [o ^ m for o in reached]

    def forward(hop):
        m, offsets = hop
        return [
            send_pot(across(o), (x, across(m))) for o in offsets for x in [cx] + mates
        ]

    hop = [i for h in hops[:1] for i in forward(h)]
    send_group(0, [0], near + far)
    send_group(0, others, near + far)

    def enter(t):
        wait_block(block[t])
        assemble(block[t])
        send_edges(0, v0, block[t], t)
        y_pass(v0, c0, block[t])

    def enter_chip():
        for t in (0, 1):
            enter(t)
        for t in (0, 1):
            edge_wait(0, t)
            z_pass(0, v0, c0, block[t], t)

    pl.when(odd == 1)(enter_chip)
    for i in hop:
        wait_pot(i)
    for h in hops[1:]:
        for i in forward(h):
            wait_pot(i)
    for i in later:
        wait_pot(i)
    sharing = share_pot()
    pl.when(odd == 0)(enter_chip)
    for t in range(2, gx):
        enter(t)
    wait_all(sharing)
    assemble_potential()
    for t in range(gx):
        before_edges(block[t])
    for t in range(2, gx - 1):
        edge_wait(0, t)
        z_pass(0, v0, c0, block[t], t)
    for t in range(1, gx - 2):
        first_x_pass(t)
    edge_wait(0, gx - 1)
    z_pass(0, v0, c0, block[gx - 1], gx - 1)
    for t in (gx - 2, gx - 1, 0):
        first_x_pass(t)

    own_out = []

    def last_x_pass(t):
        sx = block[t]

        @pl.loop(0, bx // many)
        def _(i):
            x = sx * bx + i * many
            at = pl.multiple_of(i * many * by, 8)
            for y in range(0, ny, tall):
                for g, total in enumerate(crossed(c1, x, y, along_x(v1, x, y))):
                    got = (2.0 / HALF_WIDTH) * total - v0[x + g + R, pl.ds(Y0 + y, tall), :]
                    low = y
                    while low < y + tall:
                        sy = low // by
                        high = min(y + tall, (sy + 1) * by)
                        obuf[sx, sy, pl.ds(at + g * by + low - sy * by, high - low), :] = got[
                            low - y : high - y
                        ]
                        low = high

        for dy in cross_order:
            ty = across(dy)
            n = t * gy + dy
            if n == 0:
                own_out.append(
                    pltpu.make_async_copy(obuf.at[sx, ty], out.at[:, band], lsem.at[1])
                )
                own_out[0].start()
                continue
            copy = pltpu.make_async_remote_copy(
                obuf.at[sx, ty], out.at[:, band], osend.at[0], orecv.at[0],
                device_id=(sx, ty, cz), device_id_type=MESH,
            )
            copy.start()

    done = []
    for t in list(range(1, gx)) + [0]:
        edge_wait(1, t)
        z_pass(1, v1, c1, block[t], t)
        done.append(t)
        for u in list(range(2, gx)) + [0, 1]:
            near = {u, (u + 1) % gx, (u - 1) % gx}
            if near <= set(done) and t in near:
                last_x_pass(u)
    own_out[0].wait()
    for copy in pot_out:
        copy.wait_send()
    edges = ebuf.at[:, :, :, pl.ds(0, R)]
    meet(edges, edges, hsend.at[0], hrecv.at[0, 0]).wait_send()
    sent = vin.at[pl.ds(0, gx * gy - 1)]
    meet(sent, sent, isend.at[0], orecv.at[0]).wait_send()
    meet(sent, sent, osend.at[0], orecv.at[0]).wait_send()
    meet(sent, sent, osend.at[0], orecv.at[0]).wait_recv()


def local(sizes, orbitals, potential):
    gx, gy, gz = sizes
    bands, bx, by, bz = orbitals.shape
    nx, ny = gx * bx, gy * by
    assert bands == gx * gy and gz > 1 and gx >= 4 and gx & (gx - 1) == 0
    assert gy >= 2 and gy & (gy - 1) == 0
    f32 = jnp.float32
    anywhere = pl.BlockSpec(memory_space=pl.ANY)
    dma = pltpu.SemaphoreType.DMA
    hops, mates = gy.bit_length() - 1, gx // 2 - 1
    pots = hops + mates + hops * mates + (1 + mates) * sum(2**k - 1 for k in range(1, hops))
    edge = (DEGREE, gx, 2, 8, (bx * ny + 127) // 128 * 128)
    out = pl.pallas_call(
        functools.partial(kernel, gx, gy, gz, bx, by),
        out_shape=jax.ShapeDtypeStruct((bx * by, bands, bz), f32),
        in_specs=[anywhere] * 2,
        out_specs=anywhere,
        scratch_shapes=[
            pltpu.VMEM((3 * bz + 128, 2 * bz), jnp.bfloat16),
            pltpu.VMEM((gx * gy, bx * by, bz), f32),
            pltpu.VMEM((gx, gy, bx, by, bz), f32),
            pltpu.VMEM((nx, ny, bz), f32),
            pltpu.VMEM((nx + 2 * R, ny + 16, bz), f32),
            pltpu.VMEM((nx + 2 * R, ny + 16, bz), f32),
            pltpu.VMEM((nx, ny + 16, bz), f32),
            pltpu.VMEM((nx + 2 * R, ny, bz), f32),
            pltpu.VMEM((nx + 2 * R, ny, bz), f32),
            pltpu.VMEM((nx, ny, bz), f32),
            pltpu.VMEM((gx, gy, bx * by, bz), f32),
            pltpu.VMEM(edge, f32),
            pltpu.VMEM(edge, f32),
            dma((1,)), dma((gx,)),
            dma((pots,)), dma((pots,)),
            dma((gx // 2,)), dma((gx // 2,)),
            dma((1,)), dma((DEGREE, gx)),
            dma((1,)), dma((1,)),
            dma((2,)),
        ],
        compiler_params=pltpu.CompilerParams(
            collective_id=0, has_side_effects=True, vmem_limit_bytes=48 * 1024 * 1024
        ),
    )(
        pltpu.with_memory_space_constraint(
            orbitals.transpose(1, 2, 0, 3).reshape(bx * by, bands, bz), pltpu.HBM
        ),
        pltpu.with_memory_space_constraint(potential, pltpu.HBM),
    )
    return out.reshape(bx, by, bands, bz).transpose(2, 0, 1, 3)


def solution(mesh):
    sizes = tuple(mesh.shape[a] for a in ("gx", "gy", "gz"))
    return jax.shard_map(
        functools.partial(local, sizes),
        mesh=mesh,
        in_specs=(P(None, "gx", "gy", "gz"), P("gx", "gy", "gz")),
        out_specs=P(None, "gx", "gy", "gz"),
        check_vma=False,
    )
```

```python
import functools
import math

import jax
import jax.numpy as jnp
import numpy as np
from jax import lax
from jax.experimental import pallas as pl
from jax.experimental.pallas import tpu as pltpu
from jax.sharding import PartitionSpec as P

DEGREE = 2
SECOND = (
    -5369.0 / 1800.0,
    12.0 / 7.0,
    -15.0 / 56.0,
    10.0 / 189.0,
    -1.0 / 112.0,
    2.0 / 1925.0,
    -1.0 / 16632.0,
)
FIRST = (6.0 / 7.0, -15.0 / 56.0, 5.0 / 63.0, -1.0 / 56.0, 3.0 / 385.0, -1.0 / 792.0)
METRIC = ((1.0, 0.25, 0.15), (0.25, 1.0, 0.2), (0.15, 0.2, 1.0))
CENTER = 10.5
HALF_WIDTH = 9.5
R = 6
Y0 = 8
MESH = pl.DeviceIdType.MESH


def halves(x):
    high = float(np.float32(x).astype(jnp.bfloat16))
    return high, float(np.float32(x - high).astype(jnp.bfloat16))


def bands_of(offset, part):
    out = []
    cross = [-METRIC[1][2] * c for c in FIRST]
    for table, sign in ((cross, -1.0), ([-0.5 * METRIC[2][2] * c for c in SECOND[1:]], 1.0)):
        acc = jnp.zeros(offset.shape, jnp.float32)
        for k in range(1, R + 1):
            value = halves(table[k - 1])[part]
            acc = jnp.where(offset == k, value, acc)
            acc = jnp.where(offset == -k, sign * value, acc)
        out.append(acc)
    return jnp.concatenate(out, axis=1).astype(jnp.bfloat16)


def z_matrix(bz, w_ref):
    def index(shape, dim):
        return lax.broadcasted_iota(jnp.int32, shape, dim)

    square, edge = (bz, bz), (16, bz)
    offset = index(square, 0) - index(square, 1)
    e = index(edge, 0)
    beyond = jnp.where(e < 8, e - 8, e - 8 + bz) - index(edge, 1)
    high, edge_high = bands_of(offset, 0), bands_of(beyond, 0)
    parts = [high, high, bands_of(offset, 1), edge_high, edge_high, bands_of(beyond, 1)]
    parts.append(jnp.zeros((80, 2 * bz), jnp.bfloat16))
    at = 0
    for part in parts:
        w_ref[pl.ds(at, part.shape[0]), :] = part
        at += part.shape[0]


def kernel(
    gx, gy, gz, bx, by,
    orb, pot, out,
    w_ref, vin, pin, p_ref, v0, v1, a_ref, c0, c1, s_ref, obuf, ebuf, hbuf,
    isend, irecv, psend, precv, qsend, qrecv, hsend, hrecv, osend, orecv, lsem,
):
    bz = orb.shape[-1]
    nx, ny = gx * bx, gy * by
    group = 8 // math.gcd(by, 8)
    rows = bx * ny
    padded_rows = ebuf.shape[-1]
    tall = math.gcd(ny, 8)
    cx, cy, cz = lax.axis_index("gx"), lax.axis_index("gy"), lax.axis_index("gz")
    band = cx * gy + cy
    zl, zr = lax.rem(cz + gz - 1, gz), lax.rem(cz + 1, gz)
    odd = lax.rem(cx, 2)
    chip = cx - odd
    partner = chip + 1 - odd

    def across(d):
        ty, bit = cy, 1
        while bit <= d:
            if d & bit:
                ty = ty + bit - 2 * bit * lax.rem(lax.div(cy, bit), 2)
            bit *= 2
        return ty

    far_first = list(range(gy - 1, 0, -1))

    own_pot = pltpu.make_async_copy(pot, pin.at[cx * gy + cy], lsem.at[0])
    own_pot.start()
    own_band = pltpu.make_async_copy(orb.at[:, band], vin.at[band], irecv.at[cx])
    own_band.start()
    for step in range(DEGREE):
        for t in range(gx):
            hbuf[step, t, 0, pl.ds(0, 8 - R), :] = jnp.zeros((8 - R, padded_rows), jnp.float32)
            hbuf[step, t, 1, pl.ds(R, 8 - R), :] = jnp.zeros((8 - R, padded_rows), jnp.float32)
    barrier = pltpu.get_barrier_semaphore()
    for dx in range(gx):
        for dy in range(gy):
            if dx or dy:
                pl.semaphore_signal(
                    barrier, inc=1,
                    device_id=(lax.rem(cx + dx, gx), lax.rem(cy + dy, gy), cz),
                    device_id_type=MESH,
                )
    for z in (zl, zr):
        pl.semaphore_signal(barrier, inc=1, device_id=(cx, cy, z), device_id_type=MESH)
    pl.semaphore_wait(barrier, gx * gy + 1)

    masks = []
    m = gy - 1
    while m:
        masks.append(m)
        m //= 2
    mates = [lax.rem(cx + 2 * i, gx) for i in range(1, gx // 2)]
    pot_out = []

    def send_pot(stage, y, target):
        copy = pltpu.make_async_remote_copy(
            pin.at[cx * gy + y], pin.at[cx * gy + y], psend.at[0], precv.at[stage],
            device_id=target + (cz,), device_id_type=MESH,
        )
        copy.start()
        pot_out.append(stage)

    def pots(count):
        return pin.at[pl.ds(0, count)]

    def wait_pot(stage):
        blocks = pots(pot_out.count(stage))
        meet(blocks, blocks, psend.at[0], precv.at[stage]).wait_recv()

    def share_pot():
        copies = []
        for i, x in enumerate([cx] + mates):
            copy = pltpu.make_async_remote_copy(
                pin.at[pl.ds(x * gy, gy)], pin.at[pl.ds(x * gy, gy)], qsend.at[0], qrecv.at[0],
                device_id=(partner, cy, cz), device_id_type=MESH,
            )
            copy.start()
            copies.append(copy)
        return copies

    def meet(src, dst, send, recv):
        return pltpu.make_async_remote_copy(
            src, dst, send, recv, device_id=(partner, cy, cz), device_id_type=MESH
        )

    def send_band(tx, ty):
        pltpu.make_async_remote_copy(
            orb.at[:, tx * gy + ty], vin.at[band], isend.at[0], irecv.at[cx],
            device_id=(tx, ty, cz), device_id_type=MESH,
        ).start()

    def send_group(g, pairs, ds):
        for d in ds:
            for i in pairs:
                if i or d:
                    send_band(lax.rem(chip + 2 * i + g, gx), across(d))

    def wait_block(sx):
        blocks = vin.at[pl.ds(sx * gy, gy)]
        meet(blocks, blocks, isend.at[0], irecv.at[sx]).wait_recv()

    def wrap_y(ref, x):
        ref[x, pl.ds(Y0 - R, R), :] = ref[x, pl.ds(Y0 + ny - R, R), :]
        ref[x, pl.ds(Y0 + ny, R), :] = ref[x, pl.ds(Y0, R), :]

    def wrap_x(ref, sx):
        @pl.when(sx == 0)
        def _():
            ref[pl.ds(nx + R, R)] = ref[pl.ds(R, R)]

        @pl.when(sx == gx - 1)
        def _():
            ref[pl.ds(0, R)] = ref[pl.ds(nx, R)]

    def pieces(sx, i):
        at = pl.multiple_of(i * group * by, 8)
        for sy in range(gy):
            got = vin[sx * gy + sy, pl.ds(at, group * by), :]
            for j in range(group):
                yield sy, j, got[j * by : (j + 1) * by]

    def assemble(sx):
        @pl.loop(0, bx // group)
        def _(i):
            x = sx * bx + i * group + R
            for sy, j, piece in pieces(sx, i):
                v0[x + j, pl.ds(Y0 + sy * by, by), :] = piece
            for j in range(group):
                wrap_y(v0, x + j)
        wrap_x(v0, sx)

    def assemble_potential():
        for sx in range(gx):
            @pl.loop(0, bx)
            def _(i):
                for sy in range(gy):
                    p_ref[sx * bx + i, pl.ds(sy * by, by), :] = pin[sx * gy + sy, i] + (
                        -1.5 * SECOND[0] - CENTER
                    )

    def edge_wait(step, t):
        edges = hbuf.at[step, t, :, pl.ds(0, R)]
        meet(edges, edges, hsend.at[0], hrecv.at[step, t]).wait_recv()

    def edge_copies(step, t):
        return [
            pltpu.make_async_remote_copy(
                ebuf.at[step, t, side, pl.ds(2 * side, R)],
                hbuf.at[step, t, 1 - side, pl.ds(2 * side, R)],
                hsend.at[0], hrecv.at[step, t],
                device_id=(cx, cy, z), device_id_type=MESH,
            )
            for side, z in ((0, zl), (1, zr))
        ]

    def send_edges(step, v, sx, t):
        vals = v[pl.ds(sx * bx + R, bx), pl.ds(Y0, ny), :].reshape(rows, bz)
        if padded_rows > rows:
            vals = jnp.concatenate([vals, jnp.zeros((padded_rows - rows, bz), jnp.float32)], axis=0)
        for i in range(padded_rows // 128):
            turned = vals[i * 128 : (i + 1) * 128].T
            ebuf[step, t, 0, :, pl.ds(i * 128, 128)] = turned[:8]
            ebuf[step, t, 1, :, pl.ds(i * 128, 128)] = turned[bz - 8 :]
        for copy in edge_copies(step, t):
            copy.start()

    def y_pass(v, c_ref, sx):
        @pl.loop(0, bx // group)
        def _(i):
            for j in range(group):
                x = sx * bx + i * group + j
                for y in range(0, ny, tall):
                    first = second = None
                    for k in range(1, R + 1):
                        up = v[x + R, pl.ds(Y0 + y + k, tall), :]
                        down = v[x + R, pl.ds(Y0 + y - k, tall), :]
                        f = (-METRIC[0][1] * FIRST[k - 1]) * (up - down)
                        s = (-0.5 * METRIC[1][1] * SECOND[k]) * (up + down)
                        first = f if first is None else first + f
                        second = s if second is None else second + s
                    c_ref[x + R, pl.ds(y, tall), :] = first
                    s_ref[x, pl.ds(y, tall), :] = second

    def split(x):
        high = x.astype(jnp.bfloat16)
        return high, (x - high.astype(jnp.float32)).astype(jnp.bfloat16)

    def z_pass(step, v, c_ref, sx, t):
        vals = v[pl.ds(sx * bx + R, bx), pl.ds(Y0, ny), :].reshape(rows, bz)
        high, low = split(vals)
        sides = []
        for i in range(padded_rows // 128):
            edge = jnp.concatenate(
                [hbuf[step, t, side, :, pl.ds(i * 128, 128)] for side in (0, 1)], axis=0
            )
            eh, el = (e.astype(jnp.float32) for e in split(edge))
            block = jnp.concatenate([eh, el, eh, jnp.zeros((80, 128), jnp.float32)], axis=0)
            sides.append(block.T.astype(jnp.bfloat16))
        side = jnp.concatenate(sides, axis=0)[:rows]
        got = jnp.dot(
            jnp.concatenate([high, low, high, side], axis=1), w_ref[...],
            preferred_element_type=jnp.float32,
        )
        a = got[:, :bz].reshape(bx, ny, bz)
        s_ref[pl.ds(sx * bx, bx)] += got[:, bz:].reshape(bx, ny, bz)
        c_ref[pl.ds(sx * bx + R, bx)] += (METRIC[0][2] / METRIC[1][2]) * a
        a_ref[pl.ds(sx * bx, bx), pl.ds(Y0, ny), :] = a
        for i in range(bx):
            wrap_y(a_ref, sx * bx + i)
        wrap_x(c_ref, sx)

    many = 4 if bx % 4 == 0 and 4 % group == 0 else group

    def along_x(v, x, y):
        vs = [v[x + i, pl.ds(Y0 + y, tall), :] for i in range(many + 2 * R)]
        totals = []
        for g in range(many):
            mid = g + R
            total = s_ref[x + g, pl.ds(y, tall), :] + p_ref[x + g, pl.ds(y, tall), :] * vs[mid]
            for k in range(1, R + 1):
                second = vs[mid + k] + vs[mid - k]
                total = total + (-0.5 * METRIC[0][0] * SECOND[k]) * second
            totals.append(total)
        return totals

    def crossed(c_ref, x, y, totals):
        cs = [c_ref[x + i, pl.ds(y, tall), :] for i in range(many + 2 * R)]
        out = []
        for g, total in enumerate(totals):
            mid = g + R
            for k in range(1, R + 1):
                first = (cs[mid + k] - cs[mid - k]) + (
                    a_ref[x + g, pl.ds(Y0 + y + k, tall), :]
                    - a_ref[x + g, pl.ds(Y0 + y - k, tall), :]
                )
                total = total + FIRST[k - 1] * first
            out.append(total)
        return out

    def before_edges(sx):
        @pl.loop(0, bx // many)
        def _(i):
            x = sx * bx + i * many
            for y in range(0, ny, tall):
                for g, total in enumerate(along_x(v0, x, y)):
                    s_ref[x + g, pl.ds(y, tall), :] = total

    def wait_all(copies):
        for copy in copies:
            copy.wait()

    block = [lax.rem(cx + gx + t - 2 * t * odd, gx) for t in range(gx)]

    def first_x_pass(t):
        sx = block[t]

        @pl.loop(0, bx // many)
        def _(i):
            x = sx * bx + i * many
            for y in range(0, ny, tall):
                totals = [s_ref[x + g, pl.ds(y, tall), :] for g in range(many)]
                for g, total in enumerate(crossed(c0, x, y, totals)):
                    v1[x + g + R, pl.ds(Y0 + y, tall), :] = (1.0 / HALF_WIDTH) * total
            for g in range(many):
                wrap_y(v1, x + g + R)
        wrap_x(v1, sx)
        send_edges(1, v1, sx, t)
        y_pass(v1, c1, sx)

    far = list(range(gy // 2, gy))
    near = list(range(gy // 2))
    others = list(range(1, gx // 2))
    cross_order = far + near[::-1]

    own_pot.wait()
    for d in masks:
        send_pot(0, cy, (cx, across(d)))
    for x in mates:
        send_pot(0, cy, (x, cy))
    send_band(partner, cy)
    send_group(1, [0], near + far)
    send_group(1, others, near + far)
    z_matrix(bz, w_ref)
    wait_pot(0)
    for x in mates:
        for d in masks:
            send_pot(1, across(d), (x, cy))
    reached = [0]
    hops = []
    for k, m in enumerate(masks):
        if k:
            hops.append((m, [o for o in reached if o]))
        reached = reached + [o ^ m for o in reached]

    def forward(stage, hop):
        m, offsets = hop
        for o in offsets:
            for x in [cx] + mates:
                send_pot(stage, across(o), (x, across(m)))

    for hop in hops[:1]:
        forward(2, hop)
    send_group(0, [0], near + far)
    send_group(0, others, near + far)

    def enter(t):
        wait_block(block[t])
        assemble(block[t])
        send_edges(0, v0, block[t], t)
        y_pass(v0, c0, block[t])

    def enter_chip():
        for t in (0, 1):
            enter(t)
        for t in (0, 1):
            edge_wait(0, t)
            z_pass(0, v0, c0, block[t], t)

    pl.when(odd == 1)(enter_chip)
    for k, hop in enumerate(hops):
        if k:
            forward(2 + k, hop)
        wait_pot(2 + k)
    wait_pot(1)
    share_pot()
    pl.when(odd == 0)(enter_chip)
    for t in range(2, gx):
        enter(t)
    share = pots(gx // 2 * gy)
    meet(share, share, qsend.at[0], qrecv.at[0]).wait_recv()
    assemble_potential()
    for t in range(gx):
        before_edges(block[t])
    for t in range(2, gx - 1):
        edge_wait(0, t)
        z_pass(0, v0, c0, block[t], t)
    for t in range(1, gx - 2):
        first_x_pass(t)
    edge_wait(0, gx - 1)
    z_pass(0, v0, c0, block[gx - 1], gx - 1)
    for t in (gx - 2, gx - 1, 0):
        first_x_pass(t)

    own_out = []

    def last_x_pass(t):
        sx = block[t]

        @pl.loop(0, bx // many)
        def _(i):
            x = sx * bx + i * many
            at = pl.multiple_of(i * many * by, 8)
            for y in range(0, ny, tall):
                for g, total in enumerate(crossed(c1, x, y, along_x(v1, x, y))):
                    got = (2.0 / HALF_WIDTH) * total - v0[x + g + R, pl.ds(Y0 + y, tall), :]
                    low = y
                    while low < y + tall:
                        sy = low // by
                        high = min(y + tall, (sy + 1) * by)
                        obuf[sx, sy, pl.ds(at + g * by + low - sy * by, high - low), :] = got[
                            low - y : high - y
                        ]
                        low = high

        for dy in cross_order:
            ty = across(dy)
            n = t * gy + dy
            if n == 0:
                own_out.append(
                    pltpu.make_async_copy(obuf.at[sx, ty], out.at[:, band], lsem.at[1])
                )
                own_out[0].start()
                continue
            copy = pltpu.make_async_remote_copy(
                obuf.at[sx, ty], out.at[:, band], osend.at[0], orecv.at[0],
                device_id=(sx, ty, cz), device_id_type=MESH,
            )
            copy.start()

    done = []
    for t in list(range(1, gx)) + [0]:
        edge_wait(1, t)
        z_pass(1, v1, c1, block[t], t)
        done.append(t)
        for u in list(range(2, gx)) + [0, 1]:
            near = {u, (u + 1) % gx, (u - 1) % gx}
            if near <= set(done) and t in near:
                last_x_pass(u)
    own_out[0].wait()
    meet(share, share, qsend.at[0], qrecv.at[0]).wait_send()
    meet(pots(len(pot_out)), pots(len(pot_out)), psend.at[0], qrecv.at[0]).wait_send()
    edges = ebuf.at[:, :, :, pl.ds(0, R)]
    meet(edges, edges, hsend.at[0], hrecv.at[0, 0]).wait_send()
    sent = vin.at[pl.ds(0, gx * gy - 1)]
    meet(sent, sent, isend.at[0], orecv.at[0]).wait_send()
    meet(sent, sent, osend.at[0], orecv.at[0]).wait_send()
    meet(sent, sent, osend.at[0], orecv.at[0]).wait_recv()


def local(sizes, orbitals, potential):
    gx, gy, gz = sizes
    bands, bx, by, bz = orbitals.shape
    nx, ny = gx * bx, gy * by
    assert bands == gx * gy and gz > 1 and gx >= 4 and gx & (gx - 1) == 0
    assert gy >= 2 and gy & (gy - 1) == 0
    f32 = jnp.float32
    anywhere = pl.BlockSpec(memory_space=pl.ANY)
    dma = pltpu.SemaphoreType.DMA
    edge = (DEGREE, gx, 2, 8, (bx * ny + 127) // 128 * 128)
    out = pl.pallas_call(
        functools.partial(kernel, gx, gy, gz, bx, by),
        out_shape=jax.ShapeDtypeStruct((bx * by, bands, bz), f32),
        in_specs=[anywhere] * 2,
        out_specs=anywhere,
        scratch_shapes=[
            pltpu.VMEM((3 * bz + 128, 2 * bz), jnp.bfloat16),
            pltpu.VMEM((gx * gy, bx * by, bz), f32),
            pltpu.VMEM((gx * gy, bx, by, bz), f32),
            pltpu.VMEM((nx, ny, bz), f32),
            pltpu.VMEM((nx + 2 * R, ny + 16, bz), f32),
            pltpu.VMEM((nx + 2 * R, ny + 16, bz), f32),
            pltpu.VMEM((nx, ny + 16, bz), f32),
            pltpu.VMEM((nx + 2 * R, ny, bz), f32),
            pltpu.VMEM((nx + 2 * R, ny, bz), f32),
            pltpu.VMEM((nx, ny, bz), f32),
            pltpu.VMEM((gx, gy, bx * by, bz), f32),
            pltpu.VMEM(edge, f32),
            pltpu.VMEM(edge, f32),
            dma((1,)), dma((gx,)),
            dma((1,)), dma((gy.bit_length(),)),
            dma((1,)), dma((1,)),
            dma((1,)), dma((DEGREE, gx)),
            dma((1,)), dma((1,)),
            dma((2,)),
        ],
        compiler_params=pltpu.CompilerParams(
            collective_id=0, has_side_effects=True, vmem_limit_bytes=48 * 1024 * 1024
        ),
    )(
        pltpu.with_memory_space_constraint(
            orbitals.transpose(1, 2, 0, 3).reshape(bx * by, bands, bz), pltpu.HBM
        ),
        pltpu.with_memory_space_constraint(potential, pltpu.HBM),
    )
    return out.reshape(bx, by, bands, bz).transpose(2, 0, 1, 3)


def solution(mesh):
    sizes = tuple(mesh.shape[a] for a in ("gx", "gy", "gz"))
    return jax.shard_map(
        functools.partial(local, sizes),
        mesh=mesh,
        in_specs=(P(None, "gx", "gy", "gz"), P("gx", "gy", "gz")),
        out_specs=P(None, "gx", "gy", "gz"),
        check_vma=False,
    )
```
